32 devices in a mesh: strip: 4 (over z), tile: 8 (over y, x, core).
Axes of the slice: x: 2, y: 2, z: 4, core: 2. Of those that a mesh axis runs over, the one named last changes fastest.
Arguments:
- coords: float32 [1536, 3, 128], P(('strip', 'tile')), may hold values from -0.25 to 1536.25, as said below
- displacement: float32 [1536, 3, 128], P(('strip', 'tile')), may hold values from -0.75 to 0.75
- pairs: int32 [2048, 2], P(('strip', 'tile')), may hold values from 0 to 1535, as said below
- intact: int32 [2048, 128, 128], P(('strip', 'tile')), may hold values 0 or 1
Outputs:
- force: float32 [1536, 3, 128], P(('strip', 'tile'))
The draws below stay inside these ranges and needn't reach their ends.
Inputs may be any that keep to these rules, and one draw needn't show every extreme that they name: `coords`: each point sits within 0.25 of its lattice site: tile t covers a 4 x 4 x 8 block of unit lattice sites starting at (4 (t // 384), 4 (t % 384), 0), point i at offset (i % 4, (i // 4) % 4, i // 16). `pairs`: the rows of one device (device number d = strip index * 8 + tile index) name as first tile one of the 48 tiles that this device holds, and as second tile a different one whose strip differs from the first's by at most one and whose place within its strip differs from the first's place within its strip by at most one.
All inputs are finite; a program needn't handle non-finite values. No bound on the sum of `intact` on one device may be relied on, other than what follows from the above.
Results may differ from the reference program's by a relative error of at most 0.0003.
Values sent between devices are 32-bit elements; how exact they have to be, the bound alone decides.
A program may use at most 64 MiB of HBM per device.

```python
import math
import jax
import jax.numpy as jnp
from jax import lax

TILE = 128
TPD = 48
PAIRS_DEV = 64
TILES_STRIP = 384
TILES = 1536
PAIRS = 2048
N_STRIP = 4
N_TILE = 8


def draw_coords(key, part):
    tile_ids = jnp.arange(TILES)[:, None]
    point_ids = jnp.arange(TILE)[None, :]
    across = 4 * (tile_ids // TILES_STRIP) + point_ids % 4
    along = 4 * (tile_ids % TILES_STRIP) + point_ids // 4 % 4
    depth = point_ids // 16 + 0 * tile_ids
    lattice = jnp.stack([across, along, depth], axis=1).astype(jnp.float32)
    jitter = jax.random.uniform(key, lattice.shape, jnp.float32, -0.2, 0.2)
    return lattice + jitter


def draw_pairs(key, part):
    keys = jax.random.split(jax.random.fold_in(key, 17), 3)
    rows = jnp.arange(PAIRS)
    strip_of = rows // (PAIRS_DEV * N_TILE)
    device_in_strip = rows // PAIRS_DEV % N_TILE
    first_local = device_in_strip * TPD + jax.random.randint(keys[0], (PAIRS,), 0, TPD)
    side = jax.random.randint(keys[1], (PAIRS,), -1, 2)
    offset = jax.random.randint(keys[2], (PAIRS,), -1, 2)
    second_strip = jnp.clip(strip_of + side, 0, N_STRIP - 1)
    second_local = jnp.clip(first_local + offset, 0, TILES_STRIP - 1)
    same = (second_strip == strip_of) & (second_local == first_local)
    moved_local = jnp.where(first_local + 1 < TILES_STRIP, first_local + 1, first_local - 1)
    second_local = jnp.where(same, moved_local, second_local)
    first_tile = strip_of * TILES_STRIP + first_local
    second_tile = second_strip * TILES_STRIP + second_local
    return jnp.stack([first_tile, second_tile], axis=1).astype(jnp.int32)


def touch_ends(drawn, rng, low, high):
    longest = drawn.shape.index(max(drawn.shape))
    spots = []
    for shift in (0, 1):
        where = [jax.random.randint(jax.random.fold_in(rng, axis), (), 0, length) for axis, length in enumerate(drawn.shape)]
        where[longest] = (where[longest] + shift) % drawn.shape[longest]
        spots.append(tuple(where))
    return drawn.at[spots[0]].set(low).at[spots[1]].set(high)


def block_scale(own_key, extent, shards, smallest, top_value):
    level = 1.0
    for position, parts in shards:
        draws = jax.random.uniform(jax.random.fold_in(jax.random.fold_in(own_key, 6), position), (parts,), jnp.float32, smallest / len(shards), top_value / len(shards))
        level = level * jnp.repeat(jnp.exp(draws), extent[position] // parts).reshape((-1,) + (1,) * (len(extent) - 1 - position))
    return level


def gaussian(rng, extent, deviation, limit, pieces=(), kind=jnp.bfloat16):
    result = deviation * jax.random.normal(rng, extent, jnp.float32)
    if pieces:
        result = result * block_scale(rng, extent, pieces, -0.22, 0.18)
    return jnp.clip(result, -limit, limit).astype(kind)


def setup_inputs(seed: int = 0) -> dict:
    key_list = jax.random.split(jax.random.key(seed), 5)
    return {
        "coords": draw_coords(jax.random.fold_in(key_list[4], 71), 0),
        "displacement": gaussian(key_list[1], (TILES, 3, TILE), 0.05, 0.75, ((0, 32),), jnp.float32),
        "pairs": draw_pairs(jax.random.fold_in(key_list[4], 71), 0),
        "intact": touch_ends((jax.random.randint(key_list[3], (PAIRS, TILE, TILE), 0, 8) < 7).astype(jnp.int32), jax.random.fold_in(key_list[3], 1), 0, 1),
    }


horizon = 3.0
stiffness = 2.0
onset_stretch = 0.02
final_stretch = 0.05

def block_forces(first_block, second, bond_mask):
    bond_ref = second[0:3, None, :] - first_block[0:3, :, None]
    bond_now = bond_ref + second[3:6, None, :] - first_block[3:6, :, None]
    length_ref = jnp.sqrt(lax.optimization_barrier(jnp.sum(bond_ref * bond_ref, axis=0)))
    length_now = jnp.sqrt(lax.optimization_barrier(jnp.sum(bond_now * bond_now, axis=0)))
    stretch = (length_now - length_ref) / length_ref
    influence = jnp.maximum(0.0, 1.0 - length_ref / horizon)
    soften = jnp.clip((final_stretch - stretch) / (final_stretch - onset_stretch), 0.0, 1.0)
    pull_scale = stiffness * stretch * influence * soften * bond_mask.astype(jnp.float32) / length_now
    bond_force = pull_scale[None] * bond_now
    return (lax.optimization_barrier(jnp.sum(bond_force, axis=2)), -lax.optimization_barrier(jnp.sum(bond_force, axis=1)))

def reference(coords, displacement, pairs, intact):
    point_table = jnp.concatenate([coords, displacement], axis=1)
    group_size = math.gcd(pairs.shape[0], 8)
    grouped_pairs = pairs.reshape(-1, group_size, 2)
    grouped_bonds = intact.reshape(-1, group_size, intact.shape[1], intact.shape[2])

    def visit(forces, scan_item):
        couple, bond_mask = scan_item
        first_ids = couple[:, 0].astype(jnp.int32)
        second_ids = couple[:, 1].astype(jnp.int32)
        gain_first, gain_second = jax.vmap(block_forces)(point_table[first_ids], point_table[second_ids], bond_mask)
        forces = forces.at[first_ids].add(gain_first)
        forces = forces.at[second_ids].add(gain_second)
        return (forces, None)
    zero_forces = jnp.zeros(coords.shape, coords.dtype)
    forces, unused = lax.scan(visit, zero_forces, (grouped_pairs, grouped_bonds))
    return forces
```

```python
import math

import jax
import jax.numpy as jnp
from jax import lax
from jax.experimental import pallas as pl
from jax.experimental.pallas import tpu as pltpu
from jax.sharding import PartitionSpec as P

horizon = 3.0
stiffness = 2.0
onset_stretch = 0.02
final_stretch = 0.05
span = final_stretch - onset_stretch
scale = stiffness / (horizon * span)

MESH = pl.DeviceIdType.MESH
STRIPS = (0, -1, 1)
SIDES = (-1, 1)
EDGES = tuple((es, et) for es in STRIPS for et in SIDES)
BLOCK = 8
CENTRE = (1.5, 1.5, 3.5)
DIGITS = 4


def strip_rows(per, es):
    return pl.ds(STRIPS.index(es) * per, per)


def edge_of(es, et):
    return EDGES.index((es, et))


def dot_rows(rows, matrix):
    return lax.dot_general(rows, matrix, (((1,), (0,)), ((), ())), preferred_element_type=jnp.float32)


def dot_columns(rows, matrix):
    return lax.dot_general(rows, matrix, (((1,), (1,)), ((), ())), preferred_element_type=jnp.float32)


def pieces_of(value, count=3):
    pieces = []
    for unused in range(count):
        piece = value.astype(jnp.bfloat16)
        pieces.append(piece)
        value = value - piece.astype(jnp.float32)
    return pieces


def norm2(x, y, z):
    return x * x + y * y + z * z


def locate(a, b, strip, tile, strip_tiles, per):
    here = strip * strip_tiles
    place = a - here
    beside = b - here
    over = jnp.where(beside < 0, -1, jnp.where(beside >= strip_tiles, 1, 0))
    second_place = beside - over * strip_tiles
    at = second_place - tile * per
    order = jnp.where(over == 0, 0, jnp.where(over < 0, 1, 2))
    edge = 3 * per + 2 * order
    slot = jnp.where(at < 0, edge, jnp.where(at >= per, edge + 1, order * per + at))
    across = jnp.where(over == 0, 0, 1)
    sign = jnp.where(over == 0, second_place - place, over)
    first = jnp.clip(place - tile * per, 0, per - 1)
    return place, first, slot, across, sign


def force_kernel(
    pairs_hbm, coords_hbm, displacement_hbm, bonds_hbm, out_ref,
    pairs, ends_ref, coords, displacement, edge_out, edge_in, bonds, mask, owned, folded, halves,
    features, columns, wide_ref, wide_now, near, inverse, pulls, gains, back_strip, back_edge,
    from_strip, from_edge,
    in_sem, load_sem, halo_send, halo_recv, edge_send, edge_recv, back_send, back_recv,
    back_edge_send, back_edge_recv,
):
    per, points = coords_hbm.shape[1], coords_hbm.shape[2]
    pair_count = pairs_hbm.shape[1]
    slots = coords.shape[1]
    groups = load_sem.shape[0]
    group = pair_count // groups
    half = points // 2
    batches = per // BLOCK
    strip, tile = lax.axis_index("strip"), lax.axis_index("tile")
    strips, tiles = lax.axis_size("strip"), lax.axis_size("tile")
    strip_tiles = per * tiles

    own = pl.ds(0, per)
    inputs = [
        pltpu.make_async_copy(coords_hbm, coords.at[pl.ds(0, 3), own], in_sem.at[0]),
        pltpu.make_async_copy(displacement_hbm, displacement.at[pl.ds(0, 3), own], in_sem.at[1]),
        pltpu.make_async_copy(pairs_hbm, pairs, in_sem.at[2]),
        pltpu.make_async_copy(pairs_hbm, ends_ref, in_sem.at[3]),
    ]
    for copy in inputs:
        copy.start()

    def load(g):
        part = pl.ds(g * group, group)
        return pltpu.make_async_copy(bonds_hbm.at[part], bonds.at[part], load_sem.at[g])

    for g in range(groups):
        load(g).start()

    def exists(es, et):
        s, t = strip + es, tile + et
        return (s >= 0) & (s < strips) & (t >= 0) & (t < tiles)

    around = EDGES + tuple((es, 0) for es in SIDES)
    barrier = pltpu.get_barrier_semaphore()
    for es, et in around:
        @pl.when(exists(es, et))
        def _(es=es, et=et):
            pl.semaphore_signal(
                barrier, inc=1, device_id=(strip + es, tile + et), device_id_type=MESH
            )

    def remote(source, target, send, recv, es, et):
        return pltpu.make_async_remote_copy(
            src_ref=source, dst_ref=target, send_sem=send, recv_sem=recv,
            device_id=(strip + es, tile + et), device_id_type=MESH,
        )

    def halo(which, i):
        es = SIDES[i]
        table = (coords, displacement)[which]
        part = pl.ds(0, 3)
        return remote(
            table.at[part, own], table.at[part, strip_rows(per, -es)],
            halo_send.at[2 * which + i], halo_recv.at[2 * which + i], es, 0,
        )

    def edge(i):
        es, et = EDGES[i]
        return remote(
            edge_out.at[0 if et < 0 else 1], edge_in.at[edge_of(-es, -et)],
            edge_send.at[i], edge_recv.at[i], es, et,
        )

    def back(i):
        es = SIDES[i]
        return remote(back_strip.at[i], from_strip.at[i], back_send.at[i], back_recv.at[i], es, 0)

    def edge_back(i):
        es, et = EDGES[i]
        return remote(
            back_edge.at[i], from_edge.at[i], back_edge_send.at[i], back_edge_recv.at[i], es, et
        )

    def each_side(step, opposite):
        for i, es in enumerate(SIDES):
            pl.when(exists(-es if opposite else es, 0))(lambda i=i: step(i))

    def each_edge(step, opposite):
        for i, (es, et) in enumerate(EDGES):
            here = exists(-es, -et) if opposite else exists(es, et)
            pl.when(here)(lambda i=i: step(i))

    for copy in inputs:
        copy.wait()
    for i, at in enumerate((0, per - 1)):
        for c in range(3):
            edge_out[i, c : c + 1, :] = coords[c, at : at + 1, :]
            edge_out[i, 3 + c : 4 + c, :] = displacement[c, at : at + 1, :]

    pl.semaphore_wait(barrier, sum(jnp.where(exists(es, et), 1, 0) for es, et in around))
    each_edge(lambda i: edge(i).start(), False)
    each_side(lambda i: halo(0, i).start(), False)
    each_side(lambda i: halo(1, i).start(), False)

    row = lax.broadcasted_iota(jnp.int32, (BLOCK, points), 0)
    lane = lax.broadcasted_iota(jnp.int32, (BLOCK, points), 1)
    digits = (lax.rem(lane // DIGITS, DIGITS), lax.rem(lane, DIGITS))

    place = lax.broadcasted_iota(jnp.int32, (per, points), 0) + tile * per
    bases = (
        (DIGITS * strip).astype(jnp.float32) + CENTRE[0],
        (DIGITS * place).astype(jnp.float32) + CENTRE[1],
        CENTRE[2],
    )
    for c in range(3):
        local = coords[c, 0:per] - bases[c]
        owned[:, 4 + c, :] = local
        owned[:, c, :] = local + displacement[c, 0:per]
    owned[:, 3, :] = jnp.ones((per, points), jnp.float32)
    owned[:, 7, :] = jnp.zeros((per, points), jnp.float32)

    def order_of(source):
        odd, rest = source // half, lax.rem(source, half)
        block, i = rest // BLOCK, lax.rem(rest, BLOCK)
        quarter = half // 2
        high, wide = rest // quarter, lax.rem(rest, quarter) // BLOCK
        along = 2 * BLOCK * block + BLOCK * odd + i
        across = DIGITS * BLOCK * wide + DIGITS * i + 2 * odd + high
        return along, across

    to = lax.broadcasted_iota(jnp.int32, (points, points), 1)
    picks = [
        jnp.where(lax.broadcasted_iota(jnp.int32, (points, points), 0) == source, 1.0, 0.0).astype(jnp.bfloat16)
        for source in order_of(to)
    ]
    first_half = lax.broadcasted_iota(jnp.int32, (BLOCK * BLOCK, points), 1) < half

    def fold(g, carry):
        rows = owned[pl.ds(g * BLOCK, BLOCK)].reshape(BLOCK * BLOCK, points)
        pieces = pieces_of(rows)
        for across in range(2):
            parts = [dot_rows(piece, picks[across]) for piece in pieces]
            ordered = parts[0] + (parts[1] + parts[2])
            turned = pltpu.roll(ordered, half, 1)
            base = across * per + g * BLOCK
            folded[pl.ds(base, BLOCK)] = ordered.reshape(BLOCK, BLOCK, points)
            for h in range(2):
                twice = jnp.where(first_half, ordered, turned) if h == 0 else jnp.where(first_half, turned, ordered)
                high = twice.astype(jnp.bfloat16).astype(jnp.float32)
                both = jnp.concatenate(
                    [high.reshape(BLOCK, BLOCK, points), (twice - high).reshape(BLOCK, BLOCK, points)], axis=1
                )
                features[pl.ds((2 * across + h) * per + g * BLOCK, BLOCK)] = both.astype(jnp.bfloat16)
            flat = jnp.concatenate([ordered, turned], axis=0).T
            columns[across * batches + g] = flat[:half]
        return carry

    lax.fori_loop(0, batches, fold, 0)

    def scalars(k):
        return locate(pairs[0, k], pairs[1, k], strip, tile, strip_tiles, per)

    def lanes_of(across, sign):
        digit = jnp.where(jnp.full((BLOCK, points), across) == 1, digits[1], digits[0])
        moved = digit == jnp.where(sign > 0, DIGITS - 1, 0)
        step = jnp.where(across == 1, 1, DIGITS) * (DIGITS - 1)
        shift = jnp.where(sign > 0, step, points - step)
        return moved, shift

    def merge(value, moved, shift):
        return jnp.where(moved, pltpu.roll(value, shift, 1), value)

    def prepare(k, carry):
        unused, first, unused, across, sign = scalars(k)
        moved, shift = lanes_of(across, sign)
        main = jnp.where(sign > 0, 1, 0)
        which = across * batches + first // BLOCK
        index = jnp.where(moved, (1 - main) * half, main * half) + lax.rem(first, BLOCK) * BLOCK
        sources = [columns[which, j * BLOCK : (j + 1) * BLOCK, :] for j in range(half // BLOCK)]
        for c in range(3):
            for offset, target in ((4, wide_ref), (0, wide_now)):
                for j, source in enumerate(sources):
                    target[k, c, j * BLOCK : (j + 1) * BLOCK, :] = jnp.take_along_axis(
                        source, index + (offset + c), axis=1
                    )
        is_across = jnp.full((BLOCK, points), across) == 1
        is_odd = jnp.full((BLOCK, points), main) == 1
        quarter = half // 2 // BLOCK
        for j in range(half // BLOCK):
            high, wide = j // quarter, j % quarter
            along = [bonds[k, pl.ds((2 * j + odd) * BLOCK, BLOCK)] for odd in range(2)]
            strided = [
                bonds[k, pl.ds(DIGITS * BLOCK * wide + 2 * odd + high, BLOCK, stride=DIGITS)]
                for odd in range(2)
            ]
            even, odd = (jnp.where(is_across, strided[i], along[i]) for i in range(2))
            large, small = jnp.where(is_odd, odd, even), jnp.where(is_odd, even, odd)
            held = jnp.where(moved, pltpu.roll(small, shift, 1), large)
            mask[k, j * BLOCK : (j + 1) * BLOCK] = jnp.where(held != 0, scale, 0.0)
        return carry

    def by_group(step, before):
        def run(g, carry):
            before(g)
            return lax.fori_loop(0, group, lambda i, c: step(g * group + i, c), carry, unroll=group)

        lax.fori_loop(0, groups, run, 0)

    by_group(prepare, lambda g: load(g).wait())

    def unpack_edges(which):
        table = (coords, displacement)[which]
        for i, (es, et) in enumerate(EDGES):
            @pl.when(exists(es, et))
            def _(i=i):
                for c in range(3):
                    at = 3 * per + i
                    table[c, at : at + 1, :] = edge_in[i, 3 * which + c : 3 * which + c + 1, :]

    each_edge(lambda i: edge(i).wait_recv(), True)
    unpack_edges(0)
    unpack_edges(1)
    each_side(lambda i: halo(0, i).wait_recv(), True)

    flat_coords = coords.reshape(coords.shape[0] * slots, points)
    flat_displacement = displacement.reshape(displacement.shape[0] * slots, points)
    chunk = half // 2

    def second_rows(place, slot):
        rows = flat_coords[pl.ds(slot, BLOCK, stride=slots), :]
        by = (DIGITS * place).astype(jnp.float32) + CENTRE[1]
        return rows - jnp.where(row == 0, bases[0], jnp.where(row == 1, by, bases[2]))

    def spread(rows, c):
        return jnp.broadcast_to(rows[c : c + 1], (chunk, points))

    def refer(k, carry):
        place, unused, slot, across, sign = scalars(k)
        moved, shift = lanes_of(across, sign)
        rows = merge(second_rows(place, slot), moved, shift)
        for at in range(0, half, chunk):
            part = pl.ds(at, chunk)
            ref2 = norm2(*(spread(rows, c) - wide_ref[k, c, part, :] for c in range(3)))
            inv_ref = lax.rsqrt(ref2)
            inverse[k, part] = inv_ref
            near[k, part] = jnp.maximum(0.0, horizon - ref2 * inv_ref) * mask[k, part]
        return carry

    by_group(refer, lambda g: None)

    each_side(lambda i: halo(1, i).wait_recv(), True)

    def second_now(place, slot, moved, shift):
        rows = second_rows(place, slot) + flat_displacement[pl.ds(slot, BLOCK, stride=slots), :]
        rows = jnp.where(row < 3, rows, jnp.where(row == 3, 1.0, 0.0))
        return merge(rows, moved, shift)

    def act(k, carry):
        place, first, slot, across, sign = scalars(k)
        moved, shift = lanes_of(across, sign)
        main = jnp.where(sign > 0, 1, 0)
        rows = second_now(place, slot, moved, shift)
        leads, rests = [], []
        for at in range(0, half, chunk):
            part = pl.ds(at, chunk)
            now2 = norm2(*(spread(rows, c) - wide_now[k, c, part, :] for c in range(3)))
            inv_now, inv_ref = lax.rsqrt(now2), inverse[k, part]
            soften = jnp.clip((1.0 + final_stretch) - now2 * inv_now * inv_ref, 0.0, span)
            pull = (inv_ref - inv_now) * near[k, part] * soften
            lead = pull.astype(jnp.bfloat16)
            leads.append(lead)
            rests.append((pull - lead.astype(jnp.float32)).astype(jnp.bfloat16))
        pull = jnp.concatenate(leads + rests, axis=0)
        pulls[k] = pull
        at = 2 * across * per + first
        both = jnp.concatenate([features[at + main * per], features[at + (1 - main) * per]], axis=0)
        sums = dot_rows(both, pull)
        sums = [sums[i * BLOCK : (i + 1) * BLOCK] for i in range(4)]
        gain = jnp.where(moved, sums[2] + sums[3], sums[0] + sums[1])
        gain = gain - rows * gain[3:4]
        gain = jnp.where(moved, 0.0, gain) + pltpu.roll(jnp.where(moved, gain, 0.0), points - shift, 1)
        for c in range(3):
            gains[c, pl.ds(k, 1), :] = gain[c : c + 1]
        return carry

    by_group(act, lambda g: None)

    ends = ends_ref[...]
    unused, first_ends, second_ends, across_ends, unused = locate(
        ends[0:1], ends[1:2], strip, tile, strip_tiles, per
    )

    def row_pieces():
        pieces = []
        for c in range(3):
            pieces += pieces_of(gains[c])
        return jnp.concatenate(pieces, axis=1)

    def gather(start, count, listed, pieces):
        slot = lax.broadcasted_iota(jnp.int32, (count, pair_count), 0) + start
        weight = jnp.where(slot == listed, 1.0, 0.0).astype(jnp.bfloat16)
        sums = dot_rows(weight, pieces)
        totals = []
        for c in range(3):
            parts = [sums[:, (3 * c + j) * points : (3 * c + j + 1) * points] for j in range(3)]
            totals.append(parts[0] + (parts[1] + parts[2]))
        return totals

    second_pieces = row_pieces()
    for c, total in enumerate(gather(3 * per, BLOCK, second_ends, second_pieces)):
        for i in range(len(EDGES)):
            back_edge[i, c : c + 1, :] = total[i : i + 1]
    each_edge(lambda i: edge_back(i).start(), False)
    for i, es in enumerate(SIDES):
        for c, total in enumerate(gather(STRIPS.index(es) * per, per, second_ends, second_pieces)):
            back_strip[i, c] = total
    each_side(lambda i: back(i).start(), False)
    for c, total in enumerate(gather(0, per, second_ends, second_pieces)):
        out_ref[c] = total

    def react(k, carry):
        place, first, slot, across, sign = scalars(k)
        moved, shift = lanes_of(across, sign)
        main = jnp.where(sign > 0, 1, 0)
        rows = second_now(place, slot, moved, shift)
        sides = []
        for side in (jnp.where(moved, 0.0, rows), jnp.where(moved, rows, 0.0)):
            high = side.astype(jnp.bfloat16).astype(jnp.float32)
            sides += [high, side - high]
        sums = dot_columns(jnp.concatenate(sides, axis=0).astype(jnp.bfloat16), pulls[k])
        sums = [sums[i * BLOCK : (i + 1) * BLOCK] for i in range(4)]
        large, small = (value + pltpu.roll(value, half, 1) for value in (sums[0] + sums[1], sums[2] + sums[3]))
        odd = jnp.where(lane < half, 0, 1)
        gain = jnp.where(odd == main, large, small)
        gain = gain - folded[across * per + first] * gain[3:4]
        for c in range(3):
            gains[c, pl.ds(k, 1), :] = gain[c : c + 1]
        return carry

    by_group(react, lambda g: None)

    first_pieces = row_pieces()
    sums = [
        gather(0, per, jnp.where(across_ends == across, first_ends, -1), first_pieces) for across in range(2)
    ]
    unfold = jnp.concatenate(picks, axis=1)
    for c in range(3):
        both = jnp.concatenate([sums[0][c], sums[1][c]], axis=1)
        parts = [dot_columns(piece, unfold) for piece in pieces_of(both)]
        out_ref[c] += parts[0] + (parts[1] + parts[2])

    def receive_edge(i):
        es, et = EDGES[i]
        edge_back(i).wait_recv()
        at = per - 1 if et < 0 else 0
        for c in range(3):
            out_ref[c, at : at + 1, :] += from_edge[i, c : c + 1, :]

    def receive(i):
        back(i).wait_recv()
        out_ref[...] += from_strip[i]

    each_edge(receive_edge, True)
    each_side(receive, True)
    for which in range(2):
        each_side(lambda i: halo(which, i).wait_send(), False)
    each_edge(lambda i: edge(i).wait_send(), False)
    each_edge(lambda i: edge_back(i).wait_send(), False)
    each_side(lambda i: back(i).wait_send(), False)


def on_device(coords, displacement, pairs, intact):
    per, points = coords.shape[0], coords.shape[2]
    pair_count = pairs.shape[0]
    groups = math.gcd(pair_count, 8)
    slots = 3 * per + BLOCK
    half = points // 2
    batches = per // BLOCK
    f32 = jnp.float32
    hbm = pl.BlockSpec(memory_space=pltpu.HBM)
    total = pl.pallas_call(
        force_kernel,
        in_specs=[hbm] * 4,
        out_specs=pl.BlockSpec(memory_space=pltpu.VMEM),
        out_shape=jax.ShapeDtypeStruct((3, per, points), f32),
        scratch_shapes=[
            pltpu.SMEM((2, pair_count), jnp.int32),
            pltpu.VMEM((2, pair_count), jnp.int32),
            pltpu.VMEM((BLOCK, slots, points), f32),
            pltpu.VMEM((BLOCK, slots, points), f32),
            pltpu.VMEM((2, BLOCK, points), f32),
            pltpu.VMEM((len(EDGES), BLOCK, points), f32),
            pltpu.VMEM(intact.shape, jnp.int32),
            pltpu.VMEM((pair_count, half, points), f32),
            pltpu.VMEM((per, BLOCK, points), f32),
            pltpu.VMEM((2 * per, BLOCK, points), f32),
            pltpu.VMEM((BLOCK, points), f32),
            pltpu.VMEM((4 * per, 2 * BLOCK, points), jnp.bfloat16),
            pltpu.VMEM((2 * batches, half, points), f32),
            pltpu.VMEM((pair_count, 3, half, points), f32),
            pltpu.VMEM((pair_count, 3, half, points), f32),
            pltpu.VMEM((pair_count, half, points), f32),
            pltpu.VMEM((pair_count, half, points), f32),
            pltpu.VMEM((pair_count, points, points), jnp.bfloat16),
            pltpu.VMEM((3, pair_count, points), f32),
            pltpu.VMEM((2, 3, per, points), f32),
            pltpu.VMEM((len(EDGES), BLOCK, points), f32),
            pltpu.VMEM((2, 3, per, points), f32),
            pltpu.VMEM((len(EDGES), BLOCK, points), f32),
            pltpu.SemaphoreType.DMA((4,)),
            pltpu.SemaphoreType.DMA((groups,)),
            pltpu.SemaphoreType.DMA((4,)),
            pltpu.SemaphoreType.DMA((4,)),
            pltpu.SemaphoreType.DMA((len(EDGES),)),
            pltpu.SemaphoreType.DMA((len(EDGES),)),
            pltpu.SemaphoreType.DMA((2,)),
            pltpu.SemaphoreType.DMA((2,)),
            pltpu.SemaphoreType.DMA((len(EDGES),)),
            pltpu.SemaphoreType.DMA((len(EDGES),)),
        ],
        compiler_params=pltpu.CompilerParams(
            collective_id=0, has_side_effects=True, vmem_limit_bytes=60 * 1024 * 2**10
        ),
    )(pairs.T, coords.transpose(1, 0, 2), displacement.transpose(1, 0, 2), intact)
    return jnp.transpose(total, (1, 0, 2))


def solution(mesh):
    placed = (
        P(("strip", "tile"), None, None),
        P(("strip", "tile"), None, None),
        P(("strip", "tile"), None),
        P(("strip", "tile"), None, None),
    )
    return jax.shard_map(
        on_device,
        mesh=mesh,
        in_specs=placed,
        out_specs=P(("strip", "tile"), None, None),
        check_vma=False,
    )
```

```python
import math

import jax
import jax.numpy as jnp
from jax import lax
from jax.experimental import pallas as pl
from jax.experimental.pallas import tpu as pltpu
from jax.sharding import PartitionSpec as P

horizon = 3.0
stiffness = 2.0
onset_stretch = 0.02
final_stretch = 0.05
span = final_stretch - onset_stretch
scale = stiffness / (horizon * span)

MESH = pl.DeviceIdType.MESH
STRIPS = (0, -1, 1)
SIDES = (-1, 1)
EDGES = tuple((es, et) for es in STRIPS for et in SIDES)
BLOCK = 8
CENTRE = (1.5, 1.5, 3.5)
DIGITS = 4


def strip_rows(per, es):
    return pl.ds(STRIPS.index(es) * per, per)


def edge_of(es, et):
    return EDGES.index((es, et))


def dot_rows(rows, matrix):
    return lax.dot_general(rows, matrix, (((1,), (0,)), ((), ())), preferred_element_type=jnp.float32)


def dot_columns(rows, matrix):
    return lax.dot_general(rows, matrix, (((1,), (1,)), ((), ())), preferred_element_type=jnp.float32)


def pieces_of(value, count=3):
    pieces = []
    for unused in range(count):
        piece = value.astype(jnp.bfloat16)
        pieces.append(piece)
        value = value - piece.astype(jnp.float32)
    return pieces


def norm2(x, y, z):
    return x * x + y * y + z * z


def locate(a, b, strip, tile, strip_tiles, per):
    here = strip * strip_tiles
    place = a - here
    beside = b - here
    over = jnp.where(beside < 0, -1, jnp.where(beside >= strip_tiles, 1, 0))
    second_place = beside - over * strip_tiles
    at = second_place - tile * per
    order = jnp.where(over == 0, 0, jnp.where(over < 0, 1, 2))
    edge = 3 * per + 2 * order
    slot = jnp.where(at < 0, edge, jnp.where(at >= per, edge + 1, order * per + at))
    across = jnp.where(over == 0, 0, 1)
    main = jnp.where(jnp.where(over == 0, second_place - place, over) > 0, 1, 0)
    first = jnp.clip(place - tile * per, 0, per - 1)
    return place, first, slot, across, main


def force_kernel(
    pairs_hbm, coords_hbm, displacement_hbm, bonds_hbm, out_ref,
    listed, plan, ends_ref, lanes, coords, displacement, edge_out, edge_in, bonds, mask, owned, folded,
    features, columns, wide_ref, wide_now, rows_ref, near, inverse, pulls, gains, back_strip, back_edge,
    from_strip, from_edge,
    in_sem, plan_sem, load_sem, halo_send, halo_recv, edge_send, edge_recv, back_send, back_recv,
    back_edge_send, back_edge_recv,
):
    per, points = coords_hbm.shape[1], coords_hbm.shape[2]
    pair_count = pairs_hbm.shape[1]
    slots = coords.shape[1]
    groups = load_sem.shape[0]
    group = pair_count // groups
    half = points // 2
    batches = per // BLOCK
    strip, tile = lax.axis_index("strip"), lax.axis_index("tile")
    strips, tiles = lax.axis_size("strip"), lax.axis_size("tile")
    strip_tiles = per * tiles

    own = pl.ds(0, per)
    inputs = [
        pltpu.make_async_copy(pairs_hbm, ends_ref, in_sem.at[2]),
        pltpu.make_async_copy(coords_hbm, coords.at[pl.ds(0, 3), own], in_sem.at[0]),
        pltpu.make_async_copy(displacement_hbm, displacement.at[pl.ds(0, 3), own], in_sem.at[1]),
    ]
    for copy in inputs:
        copy.start()

    def load(g):
        part = pl.ds(g * group, group)
        return pltpu.make_async_copy(bonds_hbm.at[part], bonds.at[part], load_sem.at[g])

    for g in range(groups):
        load(g).start()

    def exists(es, et):
        s, t = strip + es, tile + et
        return (s >= 0) & (s < strips) & (t >= 0) & (t < tiles)

    around = EDGES + tuple((es, 0) for es in SIDES)
    barrier = pltpu.get_barrier_semaphore()
    for es, et in around:
        @pl.when(exists(es, et))
        def _(es=es, et=et):
            pl.semaphore_signal(
                barrier, inc=1, device_id=(strip + es, tile + et), device_id_type=MESH
            )

    def remote(source, target, send, recv, es, et):
        return pltpu.make_async_remote_copy(
            src_ref=source, dst_ref=target, send_sem=send, recv_sem=recv,
            device_id=(strip + es, tile + et), device_id_type=MESH,
        )

    def halo(which, i):
        es = SIDES[i]
        table = (coords, displacement)[which]
        part = pl.ds(0, 3)
        return remote(
            table.at[part, own], table.at[part, strip_rows(per, -es)],
            halo_send.at[2 * which + i], halo_recv.at[2 * which + i], es, 0,
        )

    def edge(i):
        es, et = EDGES[i]
        return remote(
            edge_out.at[0 if et < 0 else 1], edge_in.at[edge_of(-es, -et)],
            edge_send.at[i], edge_recv.at[i], es, et,
        )

    def back(i):
        es = SIDES[i]
        return remote(back_strip.at[i], from_strip.at[i], back_send.at[i], back_recv.at[i], es, 0)

    def edge_back(i):
        es, et = EDGES[i]
        return remote(
            back_edge.at[i], from_edge.at[i], back_edge_send.at[i], back_edge_recv.at[i], es, et
        )

    def each_side(step, opposite):
        for i, es in enumerate(SIDES):
            pl.when(exists(-es if opposite else es, 0))(lambda i=i: step(i))

    def each_edge(step, opposite):
        for i, (es, et) in enumerate(EDGES):
            here = exists(-es, -et) if opposite else exists(es, et)
            pl.when(here)(lambda i=i: step(i))

    row = lax.broadcasted_iota(jnp.int32, (BLOCK, points), 0)
    lane = lax.broadcasted_iota(jnp.int32, (BLOCK, points), 1)
    digits = (lax.rem(lane // DIGITS, DIGITS), lax.rem(lane, DIGITS))
    for across in range(2):
        for main in range(2):
            moved = digits[across] == (DIGITS - 1) * main
            lanes[2 * across + main] = jnp.where(moved, 1 - main, main) * half

    inputs[0].wait()
    ends = ends_ref[...]
    place, first, slot, across, main = locate(ends[0:1], ends[1:2], strip, tile, strip_tiles, per)
    step = jnp.where(across == 1, 1, DIGITS) * (DIGITS - 1)
    entries = (
        slot, place, across * batches + first // BLOCK, lax.rem(first, BLOCK) * BLOCK,
        jnp.where(main == 1, step, points - step), 2 * across + main,
        (2 * across + main) * per + first, (2 * across + 1 - main) * per + first,
        across * per + first,
    )
    for i, entry in enumerate(entries):
        listed[i : i + 1, :] = entry
    first_ends, second_ends, across_ends = first, slot, across

    for copy in inputs[1:]:
        copy.wait()
    for i, at in enumerate((0, per - 1)):
        for c in range(3):
            edge_out[i, c : c + 1, :] = coords[c, at : at + 1, :]
            edge_out[i, 3 + c : 4 + c, :] = displacement[c, at : at + 1, :]

    places = lax.broadcasted_iota(jnp.int32, (per, points), 0) + tile * per
    bases = (
        (DIGITS * strip).astype(jnp.float32) + CENTRE[0],
        (DIGITS * places).astype(jnp.float32) + CENTRE[1],
        CENTRE[2],
    )
    for c in range(3):
        local = coords[c, 0:per] - bases[c]
        owned[:, 4 + c, :] = local
        owned[:, c, :] = local + displacement[c, 0:per]
    owned[:, 3, :] = jnp.ones((per, points), jnp.float32)
    owned[:, 7, :] = jnp.zeros((per, points), jnp.float32)

    def order_of(source):
        odd, rest = source // half, lax.rem(source, half)
        block, i = rest // BLOCK, lax.rem(rest, BLOCK)
        quarter = half // 2
        high, wide = rest // quarter, lax.rem(rest, quarter) // BLOCK
        along = 2 * BLOCK * block + BLOCK * odd + i
        across = DIGITS * BLOCK * wide + DIGITS * i + 2 * odd + high
        return along, across

    to = lax.broadcasted_iota(jnp.int32, (points, points), 1)
    picks = [
        jnp.where(lax.broadcasted_iota(jnp.int32, (points, points), 0) == source, 1.0, 0.0).astype(jnp.bfloat16)
        for source in order_of(to)
    ]
    first_half = lax.broadcasted_iota(jnp.int32, (BLOCK * BLOCK, points), 1) < half

    def fold(g, carry):
        rows = owned[pl.ds(g * BLOCK, BLOCK)].reshape(BLOCK * BLOCK, points)
        pieces = pieces_of(rows)
        for across in range(2):
            parts = [dot_rows(piece, picks[across]) for piece in pieces]
            ordered = parts[0] + (parts[1] + parts[2])
            turned = pltpu.roll(ordered, half, 1)
            base = across * per + g * BLOCK
            folded[pl.ds(base, BLOCK)] = ordered.reshape(BLOCK, BLOCK, points)
            for h in range(2):
                twice = jnp.where(first_half, ordered, turned) if h == 0 else jnp.where(first_half, turned, ordered)
                high = twice.astype(jnp.bfloat16).astype(jnp.float32)
                both = jnp.concatenate(
                    [high.reshape(BLOCK, BLOCK, points), (twice - high).reshape(BLOCK, BLOCK, points)], axis=1
                )
                features[pl.ds((2 * across + h) * per + g * BLOCK, BLOCK)] = both.astype(jnp.bfloat16)
            flat = jnp.concatenate([ordered, turned], axis=0).T
            columns[across * batches + g] = flat[:half]
        return carry

    planned = pltpu.make_async_copy(listed, plan, plan_sem)
    planned.start()
    lax.fori_loop(0, batches, fold, 0, unroll=batches)

    pl.semaphore_wait(barrier, sum(jnp.where(exists(es, et), 1, 0) for es, et in around))
    each_edge(lambda i: edge(i).start(), False)
    each_side(lambda i: halo(0, i).start(), False)
    each_side(lambda i: halo(1, i).start(), False)
    planned.wait()

    def merge(value, moved, shift):
        return jnp.where(moved, pltpu.roll(value, shift, 1), value)

    def moved_of(kind):
        main = lax.rem(kind, 2)
        return lanes[kind] != jnp.full((BLOCK, points), main * half)

    pieces_count = half // BLOCK

    def prepare(k, carry):
        which, base, kind, shift = plan[2, k], plan[3, k], plan[5, k], plan[4, k]
        index = lanes[kind] + base
        sources = [columns[which, j * BLOCK : (j + 1) * BLOCK, :] for j in range(pieces_count)]
        for c in range(3):
            for offset, target in ((4, wide_ref), (0, wide_now)):
                for j, source in enumerate(sources):
                    target[k, c, j * BLOCK : (j + 1) * BLOCK, :] = jnp.take_along_axis(
                        source, index + (offset + c), axis=1
                    )
        moved = moved_of(kind)
        is_across = jnp.full((BLOCK, points), kind // 2) == 1
        is_odd = jnp.full((BLOCK, points), lax.rem(kind, 2)) == 1
        quarter = pieces_count // 2
        larges, packed = [], 0
        for j in range(pieces_count):
            high, wide = j // quarter, j % quarter
            along = [bonds[k, pl.ds((2 * j + odd) * BLOCK, BLOCK)] for odd in range(2)]
            strided = [
                bonds[k, pl.ds(DIGITS * BLOCK * wide + 2 * odd + high, BLOCK, stride=DIGITS)]
                for odd in range(2)
            ]
            even, odd = (jnp.where(is_across, strided[i], along[i]) for i in range(2))
            larges.append(jnp.where(is_odd, odd, even))
            packed = packed + jnp.where(is_odd, even, odd) * (1 << j)
        packed = pltpu.roll(packed, shift, 1)
        for j, large in enumerate(larges):
            held = jnp.where(moved, packed & (1 << j), large)
            mask[k, j * BLOCK : (j + 1) * BLOCK] = jnp.where(held != 0, scale, 0.0)
        return carry

    def by_group(step, size):
        def run(g, carry):
            return lax.fori_loop(0, size, lambda i, c: step(g * size + i, c), carry, unroll=size)

        lax.fori_loop(0, pair_count // size, run, 0)

    for g in range(groups):
        load(g).wait()
    by_group(prepare, math.gcd(pair_count, 8))

    def unpack_edges(which):
        table = (coords, displacement)[which]
        for i, (es, et) in enumerate(EDGES):
            @pl.when(exists(es, et))
            def _(i=i):
                for c in range(3):
                    at = 3 * per + i
                    table[c, at : at + 1, :] = edge_in[i, 3 * which + c : 3 * which + c + 1, :]

    each_edge(lambda i: edge(i).wait_recv(), True)
    unpack_edges(0)
    unpack_edges(1)
    each_side(lambda i: halo(0, i).wait_recv(), True)

    flat_coords = coords.reshape(coords.shape[0] * slots, points)
    flat_displacement = displacement.reshape(displacement.shape[0] * slots, points)
    chunk = half // 2

    def spread(rows, c):
        return jnp.broadcast_to(rows[c : c + 1], (chunk, points))

    def refer(k, carry):
        slot, place, kind, shift = plan[0, k], plan[1, k], plan[5, k], plan[4, k]
        moved = moved_of(kind)
        by = (DIGITS * place).astype(jnp.float32) + CENTRE[1]
        rows = flat_coords[pl.ds(slot, BLOCK, stride=slots), :]
        rows = rows - jnp.where(row == 0, bases[0], jnp.where(row == 1, by, bases[2]))
        rows = merge(jnp.where(row < 3, rows, jnp.where(row == 3, 1.0, 0.0)), moved, shift)
        rows_ref[k] = rows
        for at in range(0, half, chunk):
            part = pl.ds(at, chunk)
            ref2 = norm2(*(spread(rows, c) - wide_ref[k, c, part, :] for c in range(3)))
            inv_ref = lax.rsqrt(ref2)
            inverse[k, part] = inv_ref
            near[k, part] = jnp.maximum(0.0, horizon - ref2 * inv_ref) * mask[k, part]
        return carry

    by_group(refer, math.gcd(pair_count, 16))

    each_side(lambda i: halo(1, i).wait_recv(), True)

    def act(k, carry):
        slot, kind, shift = plan[0, k], plan[5, k], plan[4, k]
        moved = moved_of(kind)
        shifts = jnp.where(row < 3, flat_displacement[pl.ds(slot, BLOCK, stride=slots), :], 0.0)
        rows = rows_ref[k] + merge(shifts, moved, shift)
        rows_ref[k] = rows
        leads, rests = [], []
        for at in range(0, half, chunk):
            part = pl.ds(at, chunk)
            now2 = norm2(*(spread(rows, c) - wide_now[k, c, part, :] for c in range(3)))
            inv_now, inv_ref = lax.rsqrt(now2), inverse[k, part]
            soften = jnp.clip((1.0 + final_stretch) - now2 * inv_now * inv_ref, 0.0, span)
            pull = (inv_ref - inv_now) * near[k, part] * soften
            lead = pull.astype(jnp.bfloat16)
            leads.append(lead)
            rests.append((pull - lead.astype(jnp.float32)).astype(jnp.bfloat16))
        pull = jnp.concatenate(leads + rests, axis=0)
        pulls[k] = pull
        both = jnp.concatenate([features[plan[6, k]], features[plan[7, k]]], axis=0)
        sums = dot_rows(both, pull)
        sums = [sums[i * BLOCK : (i + 1) * BLOCK] for i in range(4)]
        gain = jnp.where(moved, sums[2] + sums[3], sums[0] + sums[1])
        gain = gain - rows * gain[3:4]
        gain = jnp.where(moved, 0.0, gain) + pltpu.roll(jnp.where(moved, gain, 0.0), points - shift, 1)
        for c in range(3):
            gains[c, pl.ds(k, 1), :] = gain[c : c + 1]
        return carry

    by_group(act, math.gcd(pair_count, 32))

    def row_pieces():
        pieces = []
        for c in range(3):
            pieces += pieces_of(gains[c])
        return jnp.concatenate(pieces, axis=1)

    def gather(start, count, listed, pieces):
        slot = lax.broadcasted_iota(jnp.int32, (count, pair_count), 0) + start
        weight = jnp.where(slot == listed, 1.0, 0.0).astype(jnp.bfloat16)
        sums = dot_rows(weight, pieces)
        totals = []
        for c in range(3):
            parts = [sums[:, (3 * c + j) * points : (3 * c + j + 1) * points] for j in range(3)]
            totals.append(parts[0] + (parts[1] + parts[2]))
        return totals

    second_pieces = row_pieces()
    for c, total in enumerate(gather(3 * per, BLOCK, second_ends, second_pieces)):
        for i in range(len(EDGES)):
            back_edge[i, c : c + 1, :] = total[i : i + 1]
    each_edge(lambda i: edge_back(i).start(), False)
    for i, es in enumerate(SIDES):
        for c, total in enumerate(gather(STRIPS.index(es) * per, per, second_ends, second_pieces)):
            back_strip[i, c] = total
    each_side(lambda i: back(i).start(), False)
    for c, total in enumerate(gather(0, per, second_ends, second_pieces)):
        out_ref[c] = total

    def react(k, carry):
        kind = plan[5, k]
        moved = moved_of(kind)
        rows = rows_ref[k]
        sides = []
        for side in (jnp.where(moved, 0.0, rows), jnp.where(moved, rows, 0.0)):
            high = side.astype(jnp.bfloat16).astype(jnp.float32)
            sides += [high, side - high]
        sums = dot_columns(jnp.concatenate(sides, axis=0).astype(jnp.bfloat16), pulls[k])
        sums = [sums[i * BLOCK : (i + 1) * BLOCK] for i in range(4)]
        large, small = (value + pltpu.roll(value, half, 1) for value in (sums[0] + sums[1], sums[2] + sums[3]))
        odd = jnp.where(lane < half, 0, 1)
        gain = jnp.where(odd == jnp.full((BLOCK, points), lax.rem(kind, 2)), large, small)
        gain = gain - folded[plan[8, k]] * gain[3:4]
        for c in range(3):
            gains[c, pl.ds(k, 1), :] = gain[c : c + 1]
        return carry

    by_group(react, math.gcd(pair_count, 16))

    first_pieces = row_pieces()
    sums = [
        gather(0, per, jnp.where(across_ends == across, first_ends, -1), first_pieces) for across in range(2)
    ]
    unfold = jnp.concatenate(picks, axis=1)
    for c in range(3):
        both = jnp.concatenate([sums[0][c], sums[1][c]], axis=1)
        parts = [dot_columns(piece, unfold) for piece in pieces_of(both)]
        out_ref[c] += parts[0] + (parts[1] + parts[2])

    def receive_edge(i):
        es, et = EDGES[i]
        edge_back(i).wait_recv()
        at = per - 1 if et < 0 else 0
        for c in range(3):
            out_ref[c, at : at + 1, :] += from_edge[i, c : c + 1, :]

    def receive(i):
        back(i).wait_recv()
        out_ref[...] += from_strip[i]

    each_edge(receive_edge, True)
    each_side(receive, True)
    for which in range(2):
        each_side(lambda i: halo(which, i).wait_send(), False)
    each_edge(lambda i: edge(i).wait_send(), False)
    each_edge(lambda i: edge_back(i).wait_send(), False)
    each_side(lambda i: back(i).wait_send(), False)


def on_device(coords, displacement, pairs, intact):
    per, points = coords.shape[0], coords.shape[2]
    pair_count = pairs.shape[0]
    groups = math.gcd(pair_count, 8)
    slots = 3 * per + BLOCK
    half = points // 2
    batches = per // BLOCK
    f32 = jnp.float32
    hbm = pl.BlockSpec(memory_space=pltpu.HBM)
    total = pl.pallas_call(
        force_kernel,
        in_specs=[hbm] * 4,
        out_specs=pl.BlockSpec(memory_space=pltpu.VMEM),
        out_shape=pltpu.VMEM((3, per, points), f32),
        scratch_shapes=[
            pltpu.VMEM((2 * BLOCK, pair_count), jnp.int32),
            pltpu.SMEM((2 * BLOCK, pair_count), jnp.int32),
            pltpu.VMEM((2, pair_count), jnp.int32),
            pltpu.VMEM((4, BLOCK, points), jnp.int32),
            pltpu.VMEM((BLOCK, slots, points), f32),
            pltpu.VMEM((BLOCK, slots, points), f32),
            pltpu.VMEM((2, BLOCK, points), f32),
            pltpu.VMEM((len(EDGES), BLOCK, points), f32),
            pltpu.VMEM(intact.shape, jnp.int32),
            pltpu.VMEM((pair_count, half, points), f32),
            pltpu.VMEM((per, BLOCK, points), f32),
            pltpu.VMEM((2 * per, BLOCK, points), f32),
            pltpu.VMEM((4 * per, 2 * BLOCK, points), jnp.bfloat16),
            pltpu.VMEM((2 * batches, half, points), f32),
            pltpu.VMEM((pair_count, 3, half, points), f32),
            pltpu.VMEM((pair_count, 3, half, points), f32),
            pltpu.VMEM((pair_count, BLOCK, points), f32),
            pltpu.VMEM((pair_count, half, points), f32),
            pltpu.VMEM((pair_count, half, points), f32),
            pltpu.VMEM((pair_count, points, points), jnp.bfloat16),
            pltpu.VMEM((3, pair_count, points), f32),
            pltpu.VMEM((2, 3, per, points), f32),
            pltpu.VMEM((len(EDGES), BLOCK, points), f32),
            pltpu.VMEM((2, 3, per, points), f32),
            pltpu.VMEM((len(EDGES), BLOCK, points), f32),
            pltpu.SemaphoreType.DMA((3,)),
            pltpu.SemaphoreType.DMA,
            pltpu.SemaphoreType.DMA((groups,)),
            pltpu.SemaphoreType.DMA((4,)),
            pltpu.SemaphoreType.DMA((4,)),
            pltpu.SemaphoreType.DMA((len(EDGES),)),
            pltpu.SemaphoreType.DMA((len(EDGES),)),
            pltpu.SemaphoreType.DMA((2,)),
            pltpu.SemaphoreType.DMA((2,)),
            pltpu.SemaphoreType.DMA((len(EDGES),)),
            pltpu.SemaphoreType.DMA((len(EDGES),)),
        ],
        compiler_params=pltpu.CompilerParams(
            collective_id=0, has_side_effects=True, vmem_limit_bytes=60 * 1024 * 2**10
        ),
    )(pairs.T, coords.transpose(1, 0, 2), displacement.transpose(1, 0, 2), intact)
    return jnp.transpose(total, (1, 0, 2))


def solution(mesh):
    placed = (
        P(("strip", "tile"), None, None),
        P(("strip", "tile"), None, None),
        P(("strip", "tile"), None),
        P(("strip", "tile"), None, None),
    )
    return jax.shard_map(
        on_device,
        mesh=mesh,
        in_specs=placed,
        out_specs=P(("strip", "tile"), None, None),
        check_vma=False,
    )
```

```python
import math

import jax
import jax.numpy as jnp
from jax import lax
from jax.experimental import pallas as pl
from jax.experimental.pallas import tpu as pltpu
from jax.sharding import PartitionSpec as P

horizon = 3.0
stiffness = 2.0
onset_stretch = 0.02
final_stretch = 0.05
span = final_stretch - onset_stretch
scale = stiffness / horizon

MESH = pl.DeviceIdType.MESH
STRIPS = (0, -1, 1)
SIDES = (-1, 1)
EDGES = tuple((es, et) for es in STRIPS for et in SIDES)
AROUND = EDGES[2:] + tuple((es, 0) for es in SIDES) + EDGES[:2]
BLOCK = 8
CENTRE = (1.5, 1.5, 3.5)
DIGITS = 4
PIECES = 2
AHEAD = 2
STEP = 8


def strip_rows(per, es):
    return pl.ds(STRIPS.index(es) * per, per)


def edge_of(es, et):
    return EDGES.index((es, et))


def dot_rows(rows, matrix):
    return lax.dot_general(rows, matrix, (((1,), (0,)), ((), ())), preferred_element_type=jnp.float32)


def dot_columns(rows, matrix):
    return lax.dot_general(rows, matrix, (((1,), (1,)), ((), ())), preferred_element_type=jnp.float32)


def pieces_of(value, count):
    pieces = []
    for unused in range(count):
        piece = value.astype(jnp.bfloat16)
        pieces.append(piece)
        value = value - piece.astype(jnp.float32)
    return pieces


def norm2(x, y, z):
    return x * x + y * y + z * z


def locate(a, b, strip, tile, strip_tiles, per):
    here = strip * strip_tiles
    place = a - here
    beside = b - here
    over = jnp.where(beside < 0, -1, jnp.where(beside >= strip_tiles, 1, 0))
    second_place = beside - over * strip_tiles
    at = second_place - tile * per
    order = jnp.where(over == 0, 0, jnp.where(over < 0, 1, 2))
    edge = 3 * per + 2 * order
    slot = jnp.where(at < 0, edge, jnp.where(at >= per, edge + 1, order * per + at))
    across = jnp.where(over == 0, 0, 1)
    main = jnp.where(jnp.where(over == 0, second_place - place, over) > 0, 1, 0)
    first = jnp.clip(place - tile * per, 0, per - 1)
    return place, first, slot, across, main


def force_kernel(
    pairs_hbm, coords_hbm, displacement_hbm, bonds_hbm, out_ref,
    listed, plan, ends_ref, lanes, coords, displacement, edge_out, edge_in, bonds, reach, owned, folded,
    features, columns, wide_ref, wide_now, rows_ref, near, inverse, steep, pulls, gains, back_strip, back_edge,
    from_strip, from_edge,
    in_sem, plan_sem, load_sem, halo_send, halo_recv, edge_send, edge_recv, back_send, back_recv,
    back_edge_send, back_edge_recv,
):
    per, points = coords_hbm.shape[1], coords_hbm.shape[2]
    pair_count = pairs_hbm.shape[1]
    slots = coords.shape[1]
    groups = load_sem.shape[0]
    group = pair_count // groups
    half = points // 2
    batches = per // BLOCK
    wholes = -(-per // half)
    strip, tile = lax.axis_index("strip"), lax.axis_index("tile")
    strips, tiles = lax.axis_size("strip"), lax.axis_size("tile")
    strip_tiles = per * tiles

    def exists(es, et):
        s, t = strip + es, tile + et
        return (s >= 0) & (s < strips) & (t >= 0) & (t < tiles)

    barrier = pltpu.get_barrier_semaphore()
    for es, et in AROUND:
        @pl.when(exists(es, et))
        def _(es=es, et=et):
            pl.semaphore_signal(
                barrier, inc=1, device_id=(strip + es, tile + et), device_id_type=MESH
            )

    own = pl.ds(0, per)
    inputs = [
        pltpu.make_async_copy(pairs_hbm, ends_ref, in_sem.at[2]),
        pltpu.make_async_copy(coords_hbm, coords.at[pl.ds(0, 3), own], in_sem.at[0]),
        pltpu.make_async_copy(displacement_hbm, displacement.at[pl.ds(0, 3), own], in_sem.at[1]),
    ]
    for copy in inputs:
        copy.start()

    def load(g):
        part = pl.ds(g * group, group)
        return pltpu.make_async_copy(bonds_hbm.at[part], bonds.at[part], load_sem.at[g])

    for g in range(groups):
        load(g).start()

    def remote(source, target, send, recv, es, et):
        return pltpu.make_async_remote_copy(
            src_ref=source, dst_ref=target, send_sem=send, recv_sem=recv,
            device_id=(strip + es, tile + et), device_id_type=MESH,
        )

    def halo(which, i):
        es = SIDES[i]
        table = (coords, displacement)[which]
        part = pl.ds(0, 3)
        return remote(
            table.at[part, own], table.at[part, strip_rows(per, -es)],
            halo_send.at[2 * which + i], halo_recv.at[2 * which + i], es, 0,
        )

    def edge(i):
        es, et = EDGES[i]
        return remote(
            edge_out.at[0 if et < 0 else 1], edge_in.at[edge_of(-es, -et)],
            edge_send.at[i], edge_recv.at[i], es, et,
        )

    def back(i):
        es = SIDES[i]
        return remote(back_strip.at[i], from_strip.at[i], back_send.at[i], back_recv.at[i], es, 0)

    def edge_back(i):
        es, et = EDGES[i]
        return remote(
            back_edge.at[i], from_edge.at[i], back_edge_send.at[i], back_edge_recv.at[i], es, et
        )

    def each_side(step, opposite):
        for i, es in enumerate(SIDES):
            pl.when(exists(-es if opposite else es, 0))(lambda i=i: step(i))

    def each_edge(step, opposite):
        for i, (es, et) in enumerate(EDGES):
            here = exists(-es, -et) if opposite else exists(es, et)
            pl.when(here)(lambda i=i: step(i))

    row = lax.broadcasted_iota(jnp.int32, (BLOCK, points), 0)
    lane = lax.broadcasted_iota(jnp.int32, (BLOCK, points), 1)
    digits = (lax.rem(lane // DIGITS, DIGITS), lax.rem(lane, DIGITS))
    for across in range(2):
        for main in range(2):
            moved = digits[across] == (DIGITS - 1) * main
            lanes[2 * across + main] = jnp.where(moved, 1 - main, main) * half

    inputs[0].wait()
    ends = ends_ref[...]
    place, first, slot, across, main = locate(ends[0:1], ends[1:2], strip, tile, strip_tiles, per)
    step = jnp.where(across == 1, 1, DIGITS) * (DIGITS - 1)
    entries = (
        slot, place, across * wholes + first // half, lax.rem(first, half),
        jnp.where(main == 1, step, points - step), 2 * across + main,
        (2 * across + main) * per + first, (2 * across + 1 - main) * per + first,
        across * per + first,
    )
    for i, entry in enumerate(entries):
        listed[i : i + 1, :] = entry
    first_ends, second_ends, across_ends = first, slot, across

    for copy in inputs[1:]:
        copy.wait()
    for i, at in enumerate((0, per - 1)):
        for c in range(3):
            edge_out[i, c : c + 1, :] = coords[c, at : at + 1, :]
            edge_out[i, 3 + c : 4 + c, :] = displacement[c, at : at + 1, :]

    places = lax.broadcasted_iota(jnp.int32, (per, points), 0) + tile * per
    bases = (
        (DIGITS * strip).astype(jnp.float32) + CENTRE[0],
        (DIGITS * places).astype(jnp.float32) + CENTRE[1],
        CENTRE[2],
    )
    for c in range(3):
        local = coords[c, 0:per] - bases[c]
        owned[:, 4 + c, :] = local
        owned[:, c, :] = local + displacement[c, 0:per]
    owned[:, 3, :] = jnp.ones((per, points), jnp.float32)
    owned[:, 7, :] = jnp.zeros((per, points), jnp.float32)

    def order_of(source):
        odd, rest = source // half, lax.rem(source, half)
        block, i = rest // BLOCK, lax.rem(rest, BLOCK)
        quarter = half // 2
        high, wide = rest // quarter, lax.rem(rest, quarter) // BLOCK
        along = 2 * BLOCK * block + BLOCK * odd + i
        across = DIGITS * BLOCK * wide + DIGITS * i + 2 * odd + high
        return along, across

    to = lax.broadcasted_iota(jnp.int32, (points, points), 1)
    picks = [
        jnp.where(lax.broadcasted_iota(jnp.int32, (points, points), 0) == source, 1.0, 0.0).astype(jnp.bfloat16)
        for source in order_of(to)
    ]
    first_half = lax.broadcasted_iota(jnp.int32, (BLOCK * BLOCK, points), 1) < half

    def fold(g, carry):
        rows = owned[pl.ds(g * BLOCK, BLOCK)].reshape(BLOCK * BLOCK, points)
        pieces = pieces_of(rows, 3)
        for across in range(2):
            parts = [dot_rows(piece, picks[across]) for piece in pieces]
            ordered = parts[0] + (parts[1] + parts[2])
            turned = pltpu.roll(ordered, half, 1)
            base = across * per + g * BLOCK
            folded[pl.ds(base, BLOCK)] = ordered.reshape(BLOCK, BLOCK, points)
            for h in range(2):
                twice = jnp.where(first_half, ordered, turned) if h == 0 else jnp.where(first_half, turned, ordered)
                high = twice.astype(jnp.bfloat16).astype(jnp.float32)
                both = jnp.concatenate(
                    [high.reshape(BLOCK, BLOCK, points), (twice - high).reshape(BLOCK, BLOCK, points)], axis=1
                )
                features[pl.ds((2 * across + h) * per + g * BLOCK, BLOCK)] = both.astype(jnp.bfloat16)
        return carry

    planned = pltpu.make_async_copy(listed, plan, plan_sem)
    planned.start()
    lax.fori_loop(0, batches, fold, 0, unroll=batches)

    def merge(value, moved, shift):
        return jnp.where(moved, pltpu.roll(value, shift, 1), value)

    def moved_of(kind):
        main = lax.rem(kind, 2)
        return lanes[kind] != jnp.full((BLOCK, points), main * half)

    pieces_count = half // BLOCK

    def widen(k, offset, target):
        which, index = plan[2, k], lanes[plan[5, k]] + plan[3, k]
        for c in range(3):
            for j in range(pieces_count):
                part = pl.ds(j * BLOCK, BLOCK)
                target[k, c, part, :] = jnp.take_along_axis(columns[which, offset + c, part, :], index, axis=1)

    def prepare_now(k, carry):
        widen(k, 0, wide_now)
        return carry

    def prepare(k, carry):
        kind, shift = plan[5, k], plan[4, k]
        widen(k, 4, wide_ref)
        moved = moved_of(kind)
        is_across = jnp.full((BLOCK, points), kind // 2) == 1
        is_odd = jnp.full((BLOCK, points), lax.rem(kind, 2)) == 1
        quarter = pieces_count // 2
        larges, packed = [], 0
        for j in range(pieces_count):
            high, wide = j // quarter, j % quarter
            along = [bonds[k, pl.ds((2 * j + odd) * BLOCK, BLOCK)] for odd in range(2)]
            strided = [
                bonds[k, pl.ds(DIGITS * BLOCK * wide + 2 * odd + high, BLOCK, stride=DIGITS)]
                for odd in range(2)
            ]
            even, odd = (jnp.where(is_across, strided[i], along[i]) for i in range(2))
            larges.append(jnp.where(is_odd, odd, even))
            packed = packed + jnp.where(is_odd, even, odd) * (1 << j)
        packed = pltpu.roll(packed, shift, 1)
        for j, large in enumerate(larges):
            held = jnp.where(moved, packed & (1 << j), large)
            reach[k, j * BLOCK : (j + 1) * BLOCK] = jnp.where(held != 0, horizon, 0.0)
        return carry

    def by_group(step, size, begin=0, end=pair_count):
        def run(g, carry):
            return lax.fori_loop(0, size, lambda i, c: step(g * size + i, c), carry, unroll=size)

        lax.fori_loop(begin // size, end // size, run, 0)

    for across in range(2):
        for b in range(wholes):
            count = min(half, per - b * half)
            for c in range(BLOCK):
                if c in (3, 7):
                    continue
                ordered = folded[pl.ds(across * per + b * half, count), c, :]
                if count < half:
                    ordered = jnp.concatenate([ordered, jnp.zeros((half - count, points), jnp.float32)], axis=0)
                turned = pltpu.roll(ordered, half, 1)
                columns[across * wholes + b, c] = jnp.concatenate([ordered, turned], axis=0).T[:half]

    planned.wait()
    pl.semaphore_wait(barrier, sum(jnp.where(exists(es, et), 1, 0) for es, et in AROUND))
    each_edge(lambda i: edge(i).start(), False)
    each_side(lambda i: halo(0, i).start(), False)
    each_side(lambda i: halo(1, i).start(), False)

    for g in range(groups):
        load(g).wait()
    large_group = math.gcd(pair_count, 16)
    ahead = large_group * AHEAD
    apiece = pair_count // ahead

    def prepare_some(k, carry):
        for i in range(apiece):
            prepare(apiece * k + i, carry)
        prepare_now(k, carry)
        return carry

    by_group(prepare_some, STEP, 0, ahead)

    def unpack_edges(which):
        table = (coords, displacement)[which]
        for i, (es, et) in enumerate(EDGES):
            for c in range(3):
                at = 3 * per + i
                table[c, at : at + 1, :] = edge_in[i, 3 * which + c : 3 * which + c + 1, :]

    each_edge(lambda i: edge(i).wait_recv(), True)
    unpack_edges(0)
    unpack_edges(1)
    each_side(lambda i: halo(0, i).wait_recv(), True)

    flat_coords = coords.reshape(coords.shape[0] * slots, points)
    flat_displacement = displacement.reshape(displacement.shape[0] * slots, points)
    chunk = half // 2

    def spread(rows, c):
        return jnp.broadcast_to(rows[c : c + 1], (chunk, points))

    def refer(k, carry):
        slot, place, kind, shift = plan[0, k], plan[1, k], plan[5, k], plan[4, k]
        moved = moved_of(kind)
        by = (DIGITS * place).astype(jnp.float32) + CENTRE[1]
        rows = flat_coords[pl.ds(slot, BLOCK, stride=slots), :]
        rows = rows - jnp.where(row == 0, bases[0], jnp.where(row == 1, by, bases[2]))
        rows = merge(jnp.where(row < 3, rows, jnp.where(row == 3, 1.0, 0.0)), moved, shift)
        rows_ref[k] = rows
        for at in range(0, half, chunk):
            part = pl.ds(at, chunk)
            ref2 = norm2(*(spread(rows, c) - wide_ref[k, c, part, :] for c in range(3)))
            inv_ref = lax.rsqrt(ref2)
            inverse[k, part] = inv_ref
            steep[k, part] = inv_ref * (1.0 / span)
            near[k, part] = jnp.maximum(0.0, reach[k, part] - ref2 * inv_ref)
        return carry

    left = (pair_count - ahead) * large_group // pair_count
    each = large_group // left

    def refer_some(k, carry):
        for i in range(each):
            refer(each * k + i, carry)
        prepare_now(ahead + k, carry)
        return carry

    by_group(refer_some, 2 * left, 0, pair_count - ahead)

    each_side(lambda i: halo(1, i).wait_recv(), True)

    def act(k, carry):
        slot, kind, shift = plan[0, k], plan[5, k], plan[4, k]
        moved = moved_of(kind)
        shifts = jnp.where(row < 3, flat_displacement[pl.ds(slot, BLOCK, stride=slots), :], 0.0)
        rows = rows_ref[k] + merge(shifts, moved, shift)
        rows_ref[k] = rows
        leads, rests = [], []
        for at in range(0, half, chunk):
            part = pl.ds(at, chunk)
            now2 = norm2(*(spread(rows, c) - wide_now[k, c, part, :] for c in range(3)))
            inv_now, inv_ref = lax.rsqrt(now2), inverse[k, part]
            soften = jnp.clip((1.0 + final_stretch) / span - now2 * inv_now * steep[k, part], 0.0, 1.0)
            pull = (inv_ref - inv_now) * near[k, part] * soften
            lead = pull.astype(jnp.bfloat16)
            leads.append(lead)
            rests.append((pull - lead.astype(jnp.float32)).astype(jnp.bfloat16))
        pull = jnp.concatenate(leads + rests, axis=0)
        pulls[k] = pull
        both = jnp.concatenate([features[plan[6, k]], features[plan[7, k]]], axis=0)
        sums = dot_rows(both, pull)
        sums = [sums[i * BLOCK : (i + 1) * BLOCK] for i in range(4)]
        gain = jnp.where(moved, sums[2] + sums[3], sums[0] + sums[1])
        gain = gain - rows * gain[3:4]
        gain = jnp.where(moved, 0.0, gain) + pltpu.roll(jnp.where(moved, gain, 0.0), points - shift, 1)
        for c in range(3):
            gains[c, pl.ds(k, 1), :] = gain[c : c + 1]
        return carry

    by_group(act, math.gcd(pair_count, 64))

    def row_pieces():
        pieces = []
        for c in range(3):
            pieces += pieces_of(scale * gains[c], PIECES)
        return jnp.concatenate(pieces, axis=1)

    def gather(start, count, listed, pieces):
        slot = lax.broadcasted_iota(jnp.int32, (count, pair_count), 0) + start
        weight = jnp.where(slot == listed, 1.0, 0.0).astype(jnp.bfloat16)
        sums = dot_rows(weight, pieces)
        totals = []
        for c in range(3):
            at = PIECES * c * points
            totals.append(sums[:, at : at + points] + sums[:, at + points : at + PIECES * points])
        return totals

    second_pieces = row_pieces()
    for c, total in enumerate(gather(per, 2 * per + BLOCK, second_ends, second_pieces)):
        for i in range(len(SIDES)):
            back_strip[i, c] = total[i * per : (i + 1) * per]
        for i in range(len(EDGES)):
            back_edge[i, c : c + 1, :] = total[2 * per + i : 2 * per + i + 1]
    each_edge(lambda i: edge_back(i).start(), False)
    each_side(lambda i: back(i).start(), False)
    for c, total in enumerate(gather(0, per, second_ends, second_pieces)):
        out_ref[c] = total

    def react(k, carry):
        kind = plan[5, k]
        moved = moved_of(kind)
        rows = rows_ref[k]
        sides = []
        for side in (jnp.where(moved, 0.0, rows), jnp.where(moved, rows, 0.0)):
            high = side.astype(jnp.bfloat16).astype(jnp.float32)
            sides += [high, side - high]
        sums = dot_columns(jnp.concatenate(sides, axis=0).astype(jnp.bfloat16), pulls[k])
        sums = [sums[i * BLOCK : (i + 1) * BLOCK] for i in range(4)]
        large, small = (value + pltpu.roll(value, half, 1) for value in (sums[0] + sums[1], sums[2] + sums[3]))
        odd = jnp.where(lane < half, 0, 1)
        gain = jnp.where(odd == jnp.full((BLOCK, points), lax.rem(kind, 2)), large, small)
        gain = gain - folded[plan[8, k]] * gain[3:4]
        for c in range(3):
            gains[c, pl.ds(k, 1), :] = gain[c : c + 1]
        return carry

    by_group(react, math.gcd(pair_count, 16))

    first_pieces = row_pieces()
    sums = [
        gather(0, per, jnp.where(across_ends == across, first_ends, -1), first_pieces) for across in range(2)
    ]
    unfold = jnp.concatenate(picks, axis=1)
    for c in range(3):
        both = jnp.concatenate([sums[0][c], sums[1][c]], axis=1)
        parts = [dot_columns(piece, unfold) for piece in pieces_of(both, PIECES)]
        out_ref[c] += parts[0] + parts[1]

    for which in range(2):
        each_side(lambda i: halo(which, i).wait_send(), False)
    each_edge(lambda i: edge(i).wait_send(), False)

    def receive_edge(i):
        es, et = EDGES[i]
        edge_back(i).wait_recv()
        at = per - 1 if et < 0 else 0
        for c in range(3):
            out_ref[c, at : at + 1, :] += from_edge[i, c : c + 1, :]

    def receive(i):
        back(i).wait_recv()
        out_ref[...] += from_strip[i]

    each_edge(receive_edge, True)
    each_side(receive, True)
    each_edge(lambda i: edge_back(i).wait_send(), False)
    each_side(lambda i: back(i).wait_send(), False)


def on_device(coords, displacement, pairs, intact):
    per, points = coords.shape[0], coords.shape[2]
    pair_count = pairs.shape[0]
    groups = math.gcd(pair_count, 8)
    slots = 3 * per + BLOCK
    half = points // 2
    wholes = -(-per // half)
    f32 = jnp.float32
    hbm = pl.BlockSpec(memory_space=pltpu.HBM)
    total = pl.pallas_call(
        force_kernel,
        in_specs=[hbm] * 4,
        out_specs=pl.BlockSpec(memory_space=pltpu.VMEM),
        out_shape=pltpu.VMEM((3, per, points), f32),
        scratch_shapes=[
            pltpu.VMEM((2 * BLOCK, pair_count), jnp.int32),
            pltpu.SMEM((2 * BLOCK, pair_count), jnp.int32),
            pltpu.VMEM((2, pair_count), jnp.int32),
            pltpu.VMEM((4, BLOCK, points), jnp.int32),
            pltpu.VMEM((BLOCK, slots, points), f32),
            pltpu.VMEM((BLOCK, slots, points), f32),
            pltpu.VMEM((2, BLOCK, points), f32),
            pltpu.VMEM((len(EDGES), BLOCK, points), f32),
            pltpu.VMEM(intact.shape, jnp.int32),
            pltpu.VMEM((pair_count, half, points), f32),
            pltpu.VMEM((per, BLOCK, points), f32),
            pltpu.VMEM((2 * per, BLOCK, points), f32),
            pltpu.VMEM((4 * per, 2 * BLOCK, points), jnp.bfloat16),
            pltpu.VMEM((2 * wholes, BLOCK, half, points), f32),
            pltpu.VMEM((pair_count, 3, half, points), f32),
            pltpu.VMEM((pair_count, 3, half, points), f32),
            pltpu.VMEM((pair_count, BLOCK, points), f32),
            pltpu.VMEM((pair_count, half, points), f32),
            pltpu.VMEM((pair_count, half, points), f32),
            pltpu.VMEM((pair_count, half, points), f32),
            pltpu.VMEM((pair_count, points, points), jnp.bfloat16),
            pltpu.VMEM((3, pair_count, points), f32),
            pltpu.VMEM((2, 3, per, points), f32),
            pltpu.VMEM((len(EDGES), BLOCK, points), f32),
            pltpu.VMEM((2, 3, per, points), f32),
            pltpu.VMEM((len(EDGES), BLOCK, points), f32),
            pltpu.SemaphoreType.DMA((3,)),
            pltpu.SemaphoreType.DMA,
            pltpu.SemaphoreType.DMA((groups,)),
            pltpu.SemaphoreType.DMA((4,)),
            pltpu.SemaphoreType.DMA((4,)),
            pltpu.SemaphoreType.DMA((len(EDGES),)),
            pltpu.SemaphoreType.DMA((len(EDGES),)),
            pltpu.SemaphoreType.DMA((2,)),
            pltpu.SemaphoreType.DMA((2,)),
            pltpu.SemaphoreType.DMA((len(EDGES),)),
            pltpu.SemaphoreType.DMA((len(EDGES),)),
        ],
        compiler_params=pltpu.CompilerParams(
            collective_id=0, has_side_effects=True, vmem_limit_bytes=60 * 1024 * 2**10
        ),
    )(pairs.T, coords.transpose(1, 0, 2), displacement.transpose(1, 0, 2), intact)
    return jnp.transpose(total, (1, 0, 2))


def solution(mesh):
    placed = (
        P(("strip", "tile"), None, None),
        P(("strip", "tile"), None, None),
        P(("strip", "tile"), None),
        P(("strip", "tile"), None, None),
    )
    return jax.shard_map(
        on_device,
        mesh=mesh,
        in_specs=placed,
        out_specs=P(("strip", "tile"), None, None),
        check_vma=False,
    )
```

```python
import math

import jax
import jax.numpy as jnp
from jax import lax
from jax.experimental import pallas as pl
from jax.experimental.pallas import tpu as pltpu
from jax.sharding import PartitionSpec as P

horizon = 3.0
stiffness = 2.0
onset_stretch = 0.02
final_stretch = 0.05
span = final_stretch - onset_stretch
scale = stiffness / horizon

MESH = pl.DeviceIdType.MESH
STRIPS = (0, -1, 1)
SIDES = (-1, 1)
EDGES = tuple((es, et) for es in STRIPS for et in SIDES)
AROUND = EDGES[2:] + tuple((es, 0) for es in SIDES) + EDGES[:2]
BLOCK = 8
CENTRE = (1.5, 1.5, 3.5)
DIGITS = 4
PIECES = 2
AHEAD = 2
STEP = 8


def strip_rows(per, es):
    return pl.ds(STRIPS.index(es) * per, per)


def edge_of(es, et):
    return EDGES.index((es, et))


def dot_rows(rows, matrix):
    return lax.dot_general(rows, matrix, (((1,), (0,)), ((), ())), preferred_element_type=jnp.float32)


def dot_columns(rows, matrix):
    return lax.dot_general(rows, matrix, (((1,), (1,)), ((), ())), preferred_element_type=jnp.float32)


def pieces_of(value, count):
    pieces = []
    for unused in range(count):
        piece = value.astype(jnp.bfloat16)
        pieces.append(piece)
        value = value - piece.astype(jnp.float32)
    return pieces


def norm2(x, y, z):
    return x * x + y * y + z * z


def locate(a, b, strip, tile, strip_tiles, per):
    here = strip * strip_tiles
    place = a - here
    beside = b - here
    over = jnp.where(beside < 0, -1, jnp.where(beside >= strip_tiles, 1, 0))
    second_place = beside - over * strip_tiles
    at = second_place - tile * per
    order = jnp.where(over == 0, 0, jnp.where(over < 0, 1, 2))
    edge = 3 * per + 2 * order
    slot = jnp.where(at < 0, edge, jnp.where(at >= per, edge + 1, order * per + at))
    across = jnp.where(over == 0, 0, 1)
    main = jnp.where(jnp.where(over == 0, second_place - place, over) > 0, 1, 0)
    first = jnp.clip(place - tile * per, 0, per - 1)
    return place, first, slot, across, main


def force_kernel(
    pairs_hbm, coords_hbm, displacement_hbm, bonds_hbm, out_ref,
    listed, plan, ends_ref, lanes, coords, displacement, edge_out, edge_in, bonds, reach, owned, folded,
    features, columns, wide_ref, wide_now, rows_ref, near, inverse, steep, pulls, gains, back_strip, back_edge,
    from_strip, from_edge,
    in_sem, plan_sem, load_sem, halo_send, halo_recv, edge_send, edge_recv, back_send, back_recv,
    back_edge_send, back_edge_recv,
):
    per, points = coords_hbm.shape[1], coords_hbm.shape[2]
    pair_count = pairs_hbm.shape[1]
    slots = coords.shape[1]
    groups = load_sem.shape[0]
    group = pair_count // groups
    half = points // 2
    batches = per // BLOCK
    wholes = -(-per // half)
    strip, tile = lax.axis_index("strip"), lax.axis_index("tile")
    strips, tiles = lax.axis_size("strip"), lax.axis_size("tile")
    strip_tiles = per * tiles

    def exists(es, et):
        s, t = strip + es, tile + et
        return (s >= 0) & (s < strips) & (t >= 0) & (t < tiles)

    barrier = pltpu.get_barrier_semaphore()
    for es, et in AROUND:
        @pl.when(exists(es, et))
        def _(es=es, et=et):
            pl.semaphore_signal(
                barrier, inc=1, device_id=(strip + es, tile + et), device_id_type=MESH
            )

    own = pl.ds(0, per)
    inputs = [
        pltpu.make_async_copy(pairs_hbm, ends_ref, in_sem.at[2]),
        pltpu.make_async_copy(coords_hbm, coords.at[pl.ds(0, 3), own], in_sem.at[0]),
        pltpu.make_async_copy(displacement_hbm, displacement.at[pl.ds(0, 3), own], in_sem.at[1]),
    ]
    for copy in inputs:
        copy.start()

    def load(g):
        part = pl.ds(g * group, group)
        return pltpu.make_async_copy(bonds_hbm.at[part], bonds.at[part], load_sem.at[g])

    for g in range(groups):
        load(g).start()

    def remote(source, target, send, recv, es, et):
        return pltpu.make_async_remote_copy(
            src_ref=source, dst_ref=target, send_sem=send, recv_sem=recv,
            device_id=(strip + es, tile + et), device_id_type=MESH,
        )

    def halo(which, i):
        es = SIDES[i]
        table = (coords, displacement)[which]
        part = pl.ds(0, 3)
        return remote(
            table.at[part, own], table.at[part, strip_rows(per, -es)],
            halo_send.at[2 * which + i], halo_recv.at[2 * which + i], es, 0,
        )

    def edge(i):
        es, et = EDGES[i]
        return remote(
            edge_out.at[0 if et < 0 else 1], edge_in.at[edge_of(-es, -et)],
            edge_send.at[i], edge_recv.at[i], es, et,
        )

    def back(i):
        es = SIDES[i]
        return remote(back_strip.at[i], from_strip.at[i], back_send.at[i], back_recv.at[i], es, 0)

    def edge_back(i):
        es, et = EDGES[i]
        return remote(
            back_edge.at[i], from_edge.at[i], back_edge_send.at[i], back_edge_recv.at[i], es, et
        )

    def each_side(step, opposite):
        for i, es in enumerate(SIDES):
            pl.when(exists(-es if opposite else es, 0))(lambda i=i: step(i))

    def each_edge(step, opposite):
        for i, (es, et) in enumerate(EDGES):
            here = exists(-es, -et) if opposite else exists(es, et)
            pl.when(here)(lambda i=i: step(i))

    row = lax.broadcasted_iota(jnp.int32, (BLOCK, points), 0)
    lane = lax.broadcasted_iota(jnp.int32, (BLOCK, points), 1)
    digits = (lax.rem(lane // DIGITS, DIGITS), lax.rem(lane, DIGITS))
    for across in range(2):
        for main in range(2):
            moved = digits[across] == (DIGITS - 1) * main
            lanes[2 * across + main] = jnp.where(moved, 1 - main, main) * half

    inputs[0].wait()
    ends = ends_ref[...]
    place, first, slot, across, main = locate(ends[0:1], ends[1:2], strip, tile, strip_tiles, per)
    step = jnp.where(across == 1, 1, DIGITS) * (DIGITS - 1)
    entries = (
        slot, place, across * wholes + first // half, lax.rem(first, half),
        jnp.where(main == 1, step, points - step), 2 * across + main,
        (2 * across + main) * per + first, (2 * across + 1 - main) * per + first,
        across * per + first,
    )
    for i, entry in enumerate(entries):
        listed[i : i + 1, :] = entry
    first_ends, second_ends, across_ends = first, slot, across

    for copy in inputs[1:]:
        copy.wait()
    for i, at in enumerate((0, per - 1)):
        for c in range(3):
            edge_out[i, c : c + 1, :] = coords[c, at : at + 1, :]
            edge_out[i, 3 + c : 4 + c, :] = displacement[c, at : at + 1, :]

    planned = pltpu.make_async_copy(listed, plan, plan_sem)
    planned.start()
    pl.semaphore_wait(barrier, sum(jnp.where(exists(es, et), 1, 0) for es, et in AROUND))
    each_edge(lambda i: edge(i).start(), False)
    each_side(lambda i: halo(0, i).start(), False)
    each_side(lambda i: halo(1, i).start(), False)
    planned.wait()
    places = lax.broadcasted_iota(jnp.int32, (per, points), 0) + tile * per
    bases = (
        (DIGITS * strip).astype(jnp.float32) + CENTRE[0],
        (DIGITS * places).astype(jnp.float32) + CENTRE[1],
        CENTRE[2],
    )
    for c in range(3):
        local = coords[c, 0:per] - bases[c]
        owned[:, 4 + c, :] = local
        owned[:, c, :] = local + displacement[c, 0:per]
    owned[:, 3, :] = jnp.ones((per, points), jnp.float32)
    owned[:, 7, :] = jnp.zeros((per, points), jnp.float32)

    def order_of(source):
        odd, rest = source // half, lax.rem(source, half)
        block, i = rest // BLOCK, lax.rem(rest, BLOCK)
        quarter = half // 2
        high, wide = rest // quarter, lax.rem(rest, quarter) // BLOCK
        along = 2 * BLOCK * block + BLOCK * odd + i
        across = DIGITS * BLOCK * wide + DIGITS * i + 2 * odd + high
        return along, across

    to = lax.broadcasted_iota(jnp.int32, (points, points), 1)
    picks = [
        jnp.where(lax.broadcasted_iota(jnp.int32, (points, points), 0) == source, 1.0, 0.0).astype(jnp.bfloat16)
        for source in order_of(to)
    ]
    first_half = lax.broadcasted_iota(jnp.int32, (BLOCK * BLOCK, points), 1) < half

    def fold(g, carry):
        rows = owned[pl.ds(g * BLOCK, BLOCK)].reshape(BLOCK * BLOCK, points)
        pieces = pieces_of(rows, 3)
        for across in range(2):
            parts = [dot_rows(piece, picks[across]) for piece in pieces]
            ordered = parts[0] + (parts[1] + parts[2])
            turned = pltpu.roll(ordered, half, 1)
            base = across * per + g * BLOCK
            folded[pl.ds(base, BLOCK)] = ordered.reshape(BLOCK, BLOCK, points)
            for h in range(2):
                twice = jnp.where(first_half, ordered, turned) if h == 0 else jnp.where(first_half, turned, ordered)
                high = twice.astype(jnp.bfloat16).astype(jnp.float32)
                both = jnp.concatenate(
                    [high.reshape(BLOCK, BLOCK, points), (twice - high).reshape(BLOCK, BLOCK, points)], axis=1
                )
                features[pl.ds((2 * across + h) * per + g * BLOCK, BLOCK)] = both.astype(jnp.bfloat16)
        return carry


    def merge(value, moved, shift):
        return jnp.where(moved, pltpu.roll(value, shift, 1), value)

    def moved_of(kind):
        main = lax.rem(kind, 2)
        return lanes[kind] != jnp.full((BLOCK, points), main * half)

    pieces_count = half // BLOCK

    def widen(k, offset, target):
        which, index = plan[2, k], lanes[plan[5, k]] + plan[3, k]
        for c in range(3):
            for j in range(pieces_count):
                part = pl.ds(j * BLOCK, BLOCK)
                target[k, c, part, :] = jnp.take_along_axis(columns[which, offset + c, part, :], index, axis=1)

    def prepare_now(k, carry):
        widen(k, 0, wide_now)
        return carry

    def prepare(k, carry):
        kind, shift = plan[5, k], plan[4, k]
        widen(k, 4, wide_ref)
        moved = moved_of(kind)
        is_across = jnp.full((BLOCK, points), kind // 2) == 1
        is_odd = jnp.full((BLOCK, points), lax.rem(kind, 2)) == 1
        quarter = pieces_count // 2
        larges, packed = [], 0
        for j in range(pieces_count):
            high, wide = j // quarter, j % quarter
            along = [bonds[k, pl.ds((2 * j + odd) * BLOCK, BLOCK)] for odd in range(2)]
            strided = [
                bonds[k, pl.ds(DIGITS * BLOCK * wide + 2 * odd + high, BLOCK, stride=DIGITS)]
                for odd in range(2)
            ]
            even, odd = (jnp.where(is_across, strided[i], along[i]) for i in range(2))
            larges.append(jnp.where(is_odd, odd, even))
            packed = packed + jnp.where(is_odd, even, odd) * (1 << j)
        packed = pltpu.roll(packed, shift, 1)
        for j, large in enumerate(larges):
            held = jnp.where(moved, packed & (1 << j), large)
            reach[k, j * BLOCK : (j + 1) * BLOCK] = jnp.where(held != 0, horizon, 0.0)
        return carry

    def by_group(step, size, begin=0, end=pair_count):
        def run(g, carry):
            return lax.fori_loop(0, size, lambda i, c: step(g * size + i, c), carry, unroll=size)

        lax.fori_loop(begin // size, end // size, run, 0)

    lax.fori_loop(0, batches, fold, 0, unroll=batches)
    for across in range(2):
        for b in range(wholes):
            count = min(half, per - b * half)
            for c in range(BLOCK):
                if c in (3, 7):
                    continue
                ordered = folded[pl.ds(across * per + b * half, count), c, :]
                if count < half:
                    ordered = jnp.concatenate([ordered, jnp.zeros((half - count, points), jnp.float32)], axis=0)
                turned = pltpu.roll(ordered, half, 1)
                columns[across * wholes + b, c] = jnp.concatenate([ordered, turned], axis=0).T[:half]


    for g in range(groups):
        load(g).wait()
    large_group = math.gcd(pair_count, 16)
    ahead = large_group * AHEAD
    apiece = pair_count // ahead

    def prepare_some(k, carry):
        for i in range(apiece):
            prepare(apiece * k + i, carry)
        prepare_now(k, carry)
        return carry

    by_group(prepare_some, STEP, 0, ahead)

    def unpack_edges(which):
        table = (coords, displacement)[which]
        for i, (es, et) in enumerate(EDGES):
            for c in range(3):
                at = 3 * per + i
                table[c, at : at + 1, :] = edge_in[i, 3 * which + c : 3 * which + c + 1, :]

    each_edge(lambda i: edge(i).wait_recv(), True)
    unpack_edges(0)
    unpack_edges(1)
    each_side(lambda i: halo(0, i).wait_recv(), True)

    flat_coords = coords.reshape(coords.shape[0] * slots, points)
    flat_displacement = displacement.reshape(displacement.shape[0] * slots, points)
    chunk = half // 2

    def spread(rows, c):
        return jnp.broadcast_to(rows[c : c + 1], (chunk, points))

    def refer(k, carry):
        slot, place, kind, shift = plan[0, k], plan[1, k], plan[5, k], plan[4, k]
        moved = moved_of(kind)
        by = (DIGITS * place).astype(jnp.float32) + CENTRE[1]
        rows = flat_coords[pl.ds(slot, BLOCK, stride=slots), :]
        rows = rows - jnp.where(row == 0, bases[0], jnp.where(row == 1, by, bases[2]))
        rows = merge(jnp.where(row < 3, rows, jnp.where(row == 3, 1.0, 0.0)), moved, shift)
        rows_ref[k] = rows
        for at in range(0, half, chunk):
            part = pl.ds(at, chunk)
            ref2 = norm2(*(spread(rows, c) - wide_ref[k, c, part, :] for c in range(3)))
            inv_ref = lax.rsqrt(ref2)
            inverse[k, part] = inv_ref
            steep[k, part] = inv_ref * (1.0 / span)
            near[k, part] = jnp.maximum(0.0, reach[k, part] - ref2 * inv_ref)
        return carry

    left = (pair_count - ahead) * large_group // pair_count
    each = large_group // left

    def refer_some(k, carry):
        for i in range(each):
            refer(each * k + i, carry)
        prepare_now(ahead + k, carry)
        return carry

    by_group(refer_some, 2 * left, 0, pair_count - ahead)

    each_side(lambda i: halo(1, i).wait_recv(), True)

    def act(k, carry):
        slot, kind, shift = plan[0, k], plan[5, k], plan[4, k]
        moved = moved_of(kind)
        shifts = jnp.where(row < 3, flat_displacement[pl.ds(slot, BLOCK, stride=slots), :], 0.0)
        rows = rows_ref[k] + merge(shifts, moved, shift)
        rows_ref[k] = rows
        leads, rests = [], []
        for at in range(0, half, chunk):
            part = pl.ds(at, chunk)
            now2 = norm2(*(spread(rows, c) - wide_now[k, c, part, :] for c in range(3)))
            inv_now, inv_ref = lax.rsqrt(now2), inverse[k, part]
            soften = jnp.clip((1.0 + final_stretch) / span - now2 * inv_now * steep[k, part], 0.0, 1.0)
            pull = (inv_ref - inv_now) * near[k, part] * soften
            lead = pull.astype(jnp.bfloat16)
            leads.append(lead)
            rests.append((pull - lead.astype(jnp.float32)).astype(jnp.bfloat16))
        pull = jnp.concatenate(leads + rests, axis=0)
        pulls[k] = pull
        both = jnp.concatenate([features[plan[6, k]], features[plan[7, k]]], axis=0)
        sums = dot_rows(both, pull)
        sums = [sums[i * BLOCK : (i + 1) * BLOCK] for i in range(4)]
        gain = jnp.where(moved, sums[2] + sums[3], sums[0] + sums[1])
        gain = gain - rows * gain[3:4]
        gain = jnp.where(moved, 0.0, gain) + pltpu.roll(jnp.where(moved, gain, 0.0), points - shift, 1)
        for c in range(3):
            gains[c, pl.ds(k, 1), :] = gain[c : c + 1]
        return carry

    by_group(act, math.gcd(pair_count, 64))

    def row_pieces():
        pieces = []
        for c in range(3):
            pieces += pieces_of(scale * gains[c], PIECES)
        return jnp.concatenate(pieces, axis=1)

    def gather(start, count, listed, pieces):
        slot = lax.broadcasted_iota(jnp.int32, (count, pair_count), 0) + start
        weight = jnp.where(slot == listed, 1.0, 0.0).astype(jnp.bfloat16)
        sums = dot_rows(weight, pieces)
        totals = []
        for c in range(3):
            at = PIECES * c * points
            totals.append(sums[:, at : at + points] + sums[:, at + points : at + PIECES * points])
        return totals

    second_pieces = row_pieces()
    for c, total in enumerate(gather(per, 2 * per + BLOCK, second_ends, second_pieces)):
        for i in range(len(SIDES)):
            back_strip[i, c] = total[i * per : (i + 1) * per]
        for i in range(len(EDGES)):
            back_edge[i, c : c + 1, :] = total[2 * per + i : 2 * per + i + 1]
    each_edge(lambda i: edge_back(i).start(), False)
    each_side(lambda i: back(i).start(), False)
    for c, total in enumerate(gather(0, per, second_ends, second_pieces)):
        out_ref[c] = total

    def react(k, carry):
        kind = plan[5, k]
        moved = moved_of(kind)
        rows = rows_ref[k]
        sides = []
        for side in (jnp.where(moved, 0.0, rows), jnp.where(moved, rows, 0.0)):
            high = side.astype(jnp.bfloat16).astype(jnp.float32)
            sides += [high, side - high]
        sums = dot_columns(jnp.concatenate(sides, axis=0).astype(jnp.bfloat16), pulls[k])
        sums = [sums[i * BLOCK : (i + 1) * BLOCK] for i in range(4)]
        large, small = (value + pltpu.roll(value, half, 1) for value in (sums[0] + sums[1], sums[2] + sums[3]))
        odd = jnp.where(lane < half, 0, 1)
        gain = jnp.where(odd == jnp.full((BLOCK, points), lax.rem(kind, 2)), large, small)
        gain = gain - folded[plan[8, k]] * gain[3:4]
        for c in range(3):
            gains[c, pl.ds(k, 1), :] = gain[c : c + 1]
        return carry

    by_group(react, math.gcd(pair_count, 16))

    first_pieces = row_pieces()
    sums = [
        gather(0, per, jnp.where(across_ends == across, first_ends, -1), first_pieces) for across in range(2)
    ]
    unfold = jnp.concatenate(picks, axis=1)
    for c in range(3):
        both = jnp.concatenate([sums[0][c], sums[1][c]], axis=1)
        parts = [dot_columns(piece, unfold) for piece in pieces_of(both, PIECES)]
        out_ref[c] += parts[0] + parts[1]

    for which in range(2):
        each_side(lambda i: halo(which, i).wait_send(), False)
    each_edge(lambda i: edge(i).wait_send(), False)

    def receive_edge(i):
        es, et = EDGES[i]
        edge_back(i).wait_recv()
        at = per - 1 if et < 0 else 0
        for c in range(3):
            out_ref[c, at : at + 1, :] += from_edge[i, c : c + 1, :]

    def receive(i):
        back(i).wait_recv()
        out_ref[...] += from_strip[i]

    each_edge(receive_edge, True)
    each_side(receive, True)
    each_edge(lambda i: edge_back(i).wait_send(), False)
    each_side(lambda i: back(i).wait_send(), False)


def on_device(coords, displacement, pairs, intact):
    per, points = coords.shape[0], coords.shape[2]
    pair_count = pairs.shape[0]
    groups = math.gcd(pair_count, 8)
    slots = 3 * per + BLOCK
    half = points // 2
    wholes = -(-per // half)
    f32 = jnp.float32
    hbm = pl.BlockSpec(memory_space=pltpu.HBM)
    total = pl.pallas_call(
        force_kernel,
        in_specs=[hbm] * 4,
        out_specs=pl.BlockSpec(memory_space=pltpu.VMEM),
        out_shape=pltpu.VMEM((3, per, points), f32),
        scratch_shapes=[
            pltpu.VMEM((2 * BLOCK, pair_count), jnp.int32),
            pltpu.SMEM((2 * BLOCK, pair_count), jnp.int32),
            pltpu.VMEM((2, pair_count), jnp.int32),
            pltpu.VMEM((4, BLOCK, points), jnp.int32),
            pltpu.VMEM((BLOCK, slots, points), f32),
            pltpu.VMEM((BLOCK, slots, points), f32),
            pltpu.VMEM((2, BLOCK, points), f32),
            pltpu.VMEM((len(EDGES), BLOCK, points), f32),
            pltpu.VMEM(intact.shape, jnp.int32),
            pltpu.VMEM((pair_count, half, points), f32),
            pltpu.VMEM((per, BLOCK, points), f32),
            pltpu.VMEM((2 * per, BLOCK, points), f32),
            pltpu.VMEM((4 * per, 2 * BLOCK, points), jnp.bfloat16),
            pltpu.VMEM((2 * wholes, BLOCK, half, points), f32),
            pltpu.VMEM((pair_count, 3, half, points), f32),
            pltpu.VMEM((pair_count, 3, half, points), f32),
            pltpu.VMEM((pair_count, BLOCK, points), f32),
            pltpu.VMEM((pair_count, half, points), f32),
            pltpu.VMEM((pair_count, half, points), f32),
            pltpu.VMEM((pair_count, half, points), f32),
            pltpu.VMEM((pair_count, points, points), jnp.bfloat16),
            pltpu.VMEM((3, pair_count, points), f32),
            pltpu.VMEM((2, 3, per, points), f32),
            pltpu.VMEM((len(EDGES), BLOCK, points), f32),
            pltpu.VMEM((2, 3, per, points), f32),
            pltpu.VMEM((len(EDGES), BLOCK, points), f32),
            pltpu.SemaphoreType.DMA((3,)),
            pltpu.SemaphoreType.DMA,
            pltpu.SemaphoreType.DMA((groups,)),
            pltpu.SemaphoreType.DMA((4,)),
            pltpu.SemaphoreType.DMA((4,)),
            pltpu.SemaphoreType.DMA((len(EDGES),)),
            pltpu.SemaphoreType.DMA((len(EDGES),)),
            pltpu.SemaphoreType.DMA((2,)),
            pltpu.SemaphoreType.DMA((2,)),
            pltpu.SemaphoreType.DMA((len(EDGES),)),
            pltpu.SemaphoreType.DMA((len(EDGES),)),
        ],
        compiler_params=pltpu.CompilerParams(
            collective_id=0, has_side_effects=True, vmem_limit_bytes=60 * 1024 * 2**10
        ),
    )(pairs.T, coords.transpose(1, 0, 2), displacement.transpose(1, 0, 2), intact)
    return jnp.transpose(total, (1, 0, 2))


def solution(mesh):
    placed = (
        P(("strip", "tile"), None, None),
        P(("strip", "tile"), None, None),
        P(("strip", "tile"), None),
        P(("strip", "tile"), None, None),
    )
    return jax.shard_map(
        on_device,
        mesh=mesh,
        in_specs=placed,
        out_specs=P(("strip", "tile"), None, None),
        check_vma=False,
    )
```

```python
import math

import jax
import jax.numpy as jnp
from jax import lax
from jax.experimental import pallas as pl
from jax.experimental.pallas import tpu as pltpu
from jax.sharding import PartitionSpec as P

horizon = 3.0
stiffness = 2.0
onset_stretch = 0.02
final_stretch = 0.05
span = final_stretch - onset_stretch
scale = stiffness / horizon

MESH = pl.DeviceIdType.MESH
STRIPS = (0, -1, 1)
SIDES = (-1, 1)
EDGES = tuple((es, et) for es in STRIPS for et in SIDES)
AROUND = EDGES[2:] + tuple((es, 0) for es in SIDES) + EDGES[:2]
BLOCK = 8
CENTRE = (1.5, 1.5, 3.5)
DIGITS = 4
PIECES = 2
AHEAD = 2
STEP = 8


def strip_rows(per, es):
    return pl.ds(STRIPS.index(es) * per, per)


def edge_of(es, et):
    return EDGES.index((es, et))


def dot_rows(rows, matrix):
    return lax.dot_general(rows, matrix, (((1,), (0,)), ((), ())), preferred_element_type=jnp.float32)


def dot_columns(rows, matrix):
    return lax.dot_general(rows, matrix, (((1,), (1,)), ((), ())), preferred_element_type=jnp.float32)


def pieces_of(value, count):
    pieces = []
    for unused in range(count):
        piece = value.astype(jnp.bfloat16)
        pieces.append(piece)
        value = value - piece.astype(jnp.float32)
    return pieces


def norm2(x, y, z):
    return x * x + y * y + z * z


def locate(a, b, strip, tile, strip_tiles, per):
    here = strip * strip_tiles
    place = a - here
    beside = b - here
    over = jnp.where(beside < 0, -1, jnp.where(beside >= strip_tiles, 1, 0))
    second_place = beside - over * strip_tiles
    at = second_place - tile * per
    order = jnp.where(over == 0, 0, jnp.where(over < 0, 1, 2))
    edge = 3 * per + 2 * order
    slot = jnp.where(at < 0, edge, jnp.where(at >= per, edge + 1, order * per + at))
    across = jnp.where(over == 0, 0, 1)
    main = jnp.where(jnp.where(over == 0, second_place - place, over) > 0, 1, 0)
    first = jnp.clip(place - tile * per, 0, per - 1)
    return place, first, slot, across, main


def force_kernel(
    pairs_hbm, coords_hbm, displacement_hbm, bonds_hbm, out_ref,
    listed, plan, ends_ref, lanes, coords, displacement, edge_out, edge_in, bonds, reach, owned, folded,
    features, columns, wide_ref, wide_now, rows_ref, near, inverse, steep, pulls, gains, back_strip, back_edge,
    from_strip, from_edge,
    in_sem, plan_sem, load_sem, halo_send, halo_recv, edge_send, edge_recv, back_send, back_recv,
    back_edge_send, back_edge_recv,
):
    per, points = coords_hbm.shape[1], coords_hbm.shape[2]
    pair_count = pairs_hbm.shape[1]
    slots = coords.shape[1]
    groups = load_sem.shape[0]
    group = pair_count // groups
    half = points // 2
    batches = per // BLOCK
    wholes = -(-per // half)
    strip, tile = lax.axis_index("strip"), lax.axis_index("tile")
    strips, tiles = lax.axis_size("strip"), lax.axis_size("tile")
    strip_tiles = per * tiles

    def exists(es, et):
        s, t = strip + es, tile + et
        return (s >= 0) & (s < strips) & (t >= 0) & (t < tiles)

    barrier = pltpu.get_barrier_semaphore()
    for es, et in AROUND:
        @pl.when(exists(es, et))
        def _(es=es, et=et):
            pl.semaphore_signal(
                barrier, inc=1, device_id=(strip + es, tile + et), device_id_type=MESH
            )

    own = pl.ds(0, per)
    inputs = [
        pltpu.make_async_copy(pairs_hbm, ends_ref, in_sem.at[2]),
        pltpu.make_async_copy(coords_hbm, coords.at[pl.ds(0, 3), own], in_sem.at[0]),
        pltpu.make_async_copy(displacement_hbm, displacement.at[pl.ds(0, 3), own], in_sem.at[1]),
    ]
    for copy in inputs:
        copy.start()

    def load(g):
        part = pl.ds(g * group, group)
        return pltpu.make_async_copy(bonds_hbm.at[part], bonds.at[part], load_sem.at[g])

    for g in range(groups):
        load(g).start()

    def remote(source, target, send, recv, es, et):
        return pltpu.make_async_remote_copy(
            src_ref=source, dst_ref=target, send_sem=send, recv_sem=recv,
            device_id=(strip + es, tile + et), device_id_type=MESH,
        )

    def halo(which, i):
        es = SIDES[i]
        table = (coords, displacement)[which]
        part = pl.ds(0, 3)
        return remote(
            table.at[part, own], table.at[part, strip_rows(per, -es)],
            halo_send.at[2 * which + i], halo_recv.at[2 * which + i], es, 0,
        )

    def edge(i):
        es, et = EDGES[i]
        return remote(
            edge_out.at[0 if et < 0 else 1], edge_in.at[edge_of(-es, -et)],
            edge_send.at[i], edge_recv.at[i], es, et,
        )

    def back(i):
        es = SIDES[i]
        return remote(back_strip.at[i], from_strip.at[i], back_send.at[i], back_recv.at[i], es, 0)

    def edge_back(i):
        es, et = EDGES[i]
        return remote(
            back_edge.at[i], from_edge.at[i], back_edge_send.at[i], back_edge_recv.at[i], es, et
        )

    def each_side(step, opposite):
        for i, es in enumerate(SIDES):
            pl.when(exists(-es if opposite else es, 0))(lambda i=i: step(i))

    def each_edge(step, opposite):
        for i, (es, et) in enumerate(EDGES):
            here = exists(-es, -et) if opposite else exists(es, et)
            pl.when(here)(lambda i=i: step(i))

    row = lax.broadcasted_iota(jnp.int32, (BLOCK, points), 0)
    lane = lax.broadcasted_iota(jnp.int32, (BLOCK, points), 1)
    digits = (lax.rem(lane // DIGITS, DIGITS), lax.rem(lane, DIGITS))
    for across in range(2):
        for main in range(2):
            moved = digits[across] == (DIGITS - 1) * main
            lanes[2 * across + main] = jnp.where(moved, 1 - main, main) * half

    inputs[0].wait()
    ends = ends_ref[...]
    place, first, slot, across, main = locate(ends[0:1], ends[1:2], strip, tile, strip_tiles, per)
    step = jnp.where(across == 1, 1, DIGITS) * (DIGITS - 1)
    entries = (
        slot, place, across * wholes + first // half, lax.rem(first, half),
        jnp.where(main == 1, step, points - step), 2 * across + main,
        (2 * across + main) * per + first, (2 * across + 1 - main) * per + first,
        across * per + first,
    )
    for i, entry in enumerate(entries):
        listed[i : i + 1, :] = entry
    first_ends, second_ends, across_ends = first, slot, across

    for copy in inputs[1:]:
        copy.wait()
    for i, at in enumerate((0, per - 1)):
        for c in range(3):
            edge_out[i, c : c + 1, :] = coords[c, at : at + 1, :]
            edge_out[i, 3 + c : 4 + c, :] = displacement[c, at : at + 1, :]

    planned = pltpu.make_async_copy(listed, plan, plan_sem)
    planned.start()
    pl.semaphore_wait(barrier, sum(jnp.where(exists(es, et), 1, 0) for es, et in AROUND))
    each_edge(lambda i: edge(i).start(), False)
    each_side(lambda i: halo(0, i).start(), False)
    each_side(lambda i: halo(1, i).start(), False)
    planned.wait()
    places = lax.broadcasted_iota(jnp.int32, (per, points), 0) + tile * per
    bases = (
        (DIGITS * strip).astype(jnp.float32) + CENTRE[0],
        (DIGITS * places).astype(jnp.float32) + CENTRE[1],
        CENTRE[2],
    )
    for c in range(3):
        local = coords[c, 0:per] - bases[c]
        owned[:, 4 + c, :] = local
        owned[:, c, :] = local + displacement[c, 0:per]
    owned[:, 3, :] = jnp.ones((per, points), jnp.float32)
    owned[:, 7, :] = jnp.zeros((per, points), jnp.float32)

    def order_of(source):
        odd, rest = source // half, lax.rem(source, half)
        block, i = rest // BLOCK, lax.rem(rest, BLOCK)
        quarter = half // 2
        high, wide = rest // quarter, lax.rem(rest, quarter) // BLOCK
        along = 2 * BLOCK * block + BLOCK * odd + i
        across = DIGITS * BLOCK * wide + DIGITS * i + 2 * odd + high
        return along, across

    to = lax.broadcasted_iota(jnp.int32, (points, points), 1)
    picks = [
        jnp.where(lax.broadcasted_iota(jnp.int32, (points, points), 0) == source, 1.0, 0.0).astype(jnp.bfloat16)
        for source in order_of(to)
    ]
    first_half = lax.broadcasted_iota(jnp.int32, (BLOCK * BLOCK, points), 1) < half

    def fold(g, carry):
        rows = owned[pl.ds(g * BLOCK, BLOCK)].reshape(BLOCK * BLOCK, points)
        pieces = pieces_of(rows, 3)
        for across in range(2):
            parts = [dot_rows(piece, picks[across]) for piece in pieces]
            ordered = parts[0] + (parts[1] + parts[2])
            turned = pltpu.roll(ordered, half, 1)
            base = across * per + g * BLOCK
            folded[pl.ds(base, BLOCK)] = ordered.reshape(BLOCK, BLOCK, points)
            for h in range(2):
                twice = jnp.where(first_half, ordered, turned) if h == 0 else jnp.where(first_half, turned, ordered)
                high = twice.astype(jnp.bfloat16).astype(jnp.float32)
                both = jnp.concatenate(
                    [high.reshape(BLOCK, BLOCK, points), (twice - high).reshape(BLOCK, BLOCK, points)], axis=1
                )
                features[pl.ds((2 * across + h) * per + g * BLOCK, BLOCK)] = both.astype(jnp.bfloat16)
        return carry


    def merge(value, moved, shift):
        return jnp.where(moved, pltpu.roll(value, shift, 1), value)

    def moved_of(kind):
        main = lax.rem(kind, 2)
        return lanes[kind] != jnp.full((BLOCK, points), main * half)

    pieces_count = half // BLOCK

    def widen(k, offset, target):
        which, index = plan[2, k], lanes[plan[5, k]] + plan[3, k]
        for c in range(3):
            for j in range(pieces_count):
                part = pl.ds(j * BLOCK, BLOCK)
                target[k, c, part, :] = jnp.take_along_axis(columns[which, offset + c, part, :], index, axis=1)

    def prepare_now(k, carry):
        widen(k, 0, wide_now)
        return carry

    def prepare(k, carry):
        kind, shift = plan[5, k], plan[4, k]
        widen(k, 4, wide_ref)
        moved = moved_of(kind)
        is_across = jnp.full((BLOCK, points), kind // 2) == 1
        is_odd = jnp.full((BLOCK, points), lax.rem(kind, 2)) == 1
        quarter = pieces_count // 2
        larges, packed = [], 0
        for j in range(pieces_count):
            high, wide = j // quarter, j % quarter
            along = [bonds[k, pl.ds((2 * j + odd) * BLOCK, BLOCK)] for odd in range(2)]
            strided = [
                bonds[k, pl.ds(DIGITS * BLOCK * wide + 2 * odd + high, BLOCK, stride=DIGITS)]
                for odd in range(2)
            ]
            even, odd = (jnp.where(is_across, strided[i], along[i]) for i in range(2))
            larges.append(jnp.where(is_odd, odd, even))
            packed = packed + jnp.where(is_odd, even, odd) * (1 << j)
        packed = pltpu.roll(packed, shift, 1)
        for j, large in enumerate(larges):
            held = jnp.where(moved, packed & (1 << j), large)
            reach[k, j * BLOCK : (j + 1) * BLOCK] = jnp.where(held != 0, horizon, 0.0)
        return carry

    def by_group(step, size, begin=0, end=pair_count):
        def run(g, carry):
            return lax.fori_loop(0, size, lambda i, c: step(g * size + i, c), carry, unroll=size)

        lax.fori_loop(begin // size, end // size, run, 0)

    lax.fori_loop(0, batches, fold, 0, unroll=batches)
    for across in range(2):
        for b in range(wholes):
            count = min(half, per - b * half)
            for c in range(BLOCK):
                if c in (3, 7):
                    continue
                ordered = folded[pl.ds(across * per + b * half, count), c, :]
                if count < half:
                    ordered = jnp.concatenate([ordered, jnp.zeros((half - count, points), jnp.float32)], axis=0)
                turned = pltpu.roll(ordered, half, 1)
                columns[across * wholes + b, c] = jnp.concatenate([ordered, turned], axis=0).T[:half]


    for g in range(groups):
        load(g).wait()
    large_group = math.gcd(pair_count, 16)
    ahead = large_group * AHEAD
    apiece = pair_count // ahead

    def prepare_some(k, carry):
        for i in range(apiece):
            prepare(apiece * k + i, carry)
        prepare_now(k, carry)
        return carry

    by_group(prepare_some, STEP, 0, ahead)

    def unpack_edges(which):
        table = (coords, displacement)[which]
        for i, (es, et) in enumerate(EDGES):
            for c in range(3):
                at = 3 * per + i
                table[c, at : at + 1, :] = edge_in[i, 3 * which + c : 3 * which + c + 1, :]

    each_edge(lambda i: edge(i).wait_recv(), True)
    unpack_edges(0)
    unpack_edges(1)
    each_side(lambda i: halo(0, i).wait_recv(), True)

    flat_coords = coords.reshape(coords.shape[0] * slots, points)
    flat_displacement = displacement.reshape(displacement.shape[0] * slots, points)
    chunk = half // 2

    def spread(rows, c):
        return jnp.broadcast_to(rows[c : c + 1], (chunk, points))

    def refer(k, carry):
        slot, place, kind, shift = plan[0, k], plan[1, k], plan[5, k], plan[4, k]
        moved = moved_of(kind)
        by = (DIGITS * place).astype(jnp.float32) + CENTRE[1]
        rows = flat_coords[pl.ds(slot, BLOCK, stride=slots), :]
        rows = rows - jnp.where(row == 0, bases[0], jnp.where(row == 1, by, bases[2]))
        rows = merge(jnp.where(row < 3, rows, jnp.where(row == 3, 1.0, 0.0)), moved, shift)
        rows_ref[k] = rows
        for at in range(0, half, chunk):
            part = pl.ds(at, chunk)
            ref2 = norm2(*(spread(rows, c) - wide_ref[k, c, part, :] for c in range(3)))
            inv_ref = lax.rsqrt(ref2)
            inverse[k, part] = inv_ref
            steep[k, part] = inv_ref * (1.0 / span)
            near[k, part] = jnp.maximum(0.0, reach[k, part] - ref2 * inv_ref)
        return carry

    left = (pair_count - ahead) * large_group // pair_count
    each = large_group // left

    def refer_some(k, carry):
        for i in range(each):
            refer(each * k + i, carry)
        prepare_now(ahead + k, carry)
        return carry

    by_group(refer_some, 2 * left, 0, pair_count - ahead)

    each_side(lambda i: halo(1, i).wait_recv(), True)

    def act(k, carry):
        slot, kind, shift = plan[0, k], plan[5, k], plan[4, k]
        moved = moved_of(kind)
        shifts = jnp.where(row < 3, flat_displacement[pl.ds(slot, BLOCK, stride=slots), :], 0.0)
        rows = rows_ref[k] + merge(shifts, moved, shift)
        rows_ref[k] = rows
        leads, rests = [], []
        for at in range(0, half, chunk):
            part = pl.ds(at, chunk)
            now2 = norm2(*(spread(rows, c) - wide_now[k, c, part, :] for c in range(3)))
            inv_now, inv_ref = lax.rsqrt(now2), inverse[k, part]
            soften = jnp.clip((1.0 + final_stretch) / span - now2 * inv_now * steep[k, part], 0.0, 1.0)
            pull = (inv_ref - inv_now) * near[k, part] * soften
            lead = pull.astype(jnp.bfloat16)
            leads.append(lead)
            rests.append((pull - lead.astype(jnp.float32)).astype(jnp.bfloat16))
        pull = jnp.concatenate(leads + rests, axis=0)
        pulls[k] = pull
        both = jnp.concatenate([features[plan[6, k]], features[plan[7, k]]], axis=0)
        sums = dot_rows(both, pull)
        sums = [sums[i * BLOCK : (i + 1) * BLOCK] for i in range(4)]
        gain = jnp.where(moved, sums[2] + sums[3], sums[0] + sums[1])
        gain = gain - rows * gain[3:4]
        gain = jnp.where(moved, 0.0, gain) + pltpu.roll(jnp.where(moved, gain, 0.0), points - shift, 1)
        for c in range(3):
            gains[c, pl.ds(k, 1), :] = gain[c : c + 1]
        return carry

    by_group(act, math.gcd(pair_count, 64))

    def row_pieces():
        pieces = []
        for c in range(3):
            pieces += pieces_of(scale * gains[c], PIECES)
        return jnp.concatenate(pieces, axis=1)

    def gather(start, count, listed, pieces):
        slot = lax.broadcasted_iota(jnp.int32, (count, pair_count), 0) + start
        weight = jnp.where(slot == listed, 1.0, 0.0).astype(jnp.bfloat16)
        sums = dot_rows(weight, pieces)
        totals = []
        for c in range(3):
            at = PIECES * c * points
            totals.append(sums[:, at : at + points] + sums[:, at + points : at + PIECES * points])
        return totals

    second_pieces = row_pieces()
    for c, total in enumerate(gather(3 * per, BLOCK, second_ends, second_pieces)):
        for i in range(len(EDGES)):
            back_edge[i, c : c + 1, :] = total[i : i + 1]
    each_edge(lambda i: edge_back(i).start(), False)
    for c, total in enumerate(gather(per, 2 * per, second_ends, second_pieces)):
        for i in range(len(SIDES)):
            back_strip[i, c] = total[i * per : (i + 1) * per]
    each_side(lambda i: back(i).start(), False)
    for c, total in enumerate(gather(0, per, second_ends, second_pieces)):
        out_ref[c] = total

    def react(k, carry):
        kind = plan[5, k]
        moved = moved_of(kind)
        rows = rows_ref[k]
        sides = []
        for side in (jnp.where(moved, 0.0, rows), jnp.where(moved, rows, 0.0)):
            high = side.astype(jnp.bfloat16).astype(jnp.float32)
            sides += [high, side - high]
        sums = dot_columns(jnp.concatenate(sides, axis=0).astype(jnp.bfloat16), pulls[k])
        sums = [sums[i * BLOCK : (i + 1) * BLOCK] for i in range(4)]
        large, small = (value + pltpu.roll(value, half, 1) for value in (sums[0] + sums[1], sums[2] + sums[3]))
        odd = jnp.where(lane < half, 0, 1)
        gain = jnp.where(odd == jnp.full((BLOCK, points), lax.rem(kind, 2)), large, small)
        gain = gain - folded[plan[8, k]] * gain[3:4]
        for c in range(3):
            gains[c, pl.ds(k, 1), :] = gain[c : c + 1]
        return carry

    by_group(react, math.gcd(pair_count, 16))

    first_pieces = row_pieces()
    sums = [
        gather(0, per, jnp.where(across_ends == across, first_ends, -1), first_pieces) for across in range(2)
    ]
    unfold = jnp.concatenate(picks, axis=1)
    for c in range(3):
        both = jnp.concatenate([sums[0][c], sums[1][c]], axis=1)
        parts = [dot_columns(piece, unfold) for piece in pieces_of(both, PIECES)]
        out_ref[c] += parts[0] + parts[1]

    for which in range(2):
        each_side(lambda i: halo(which, i).wait_send(), False)
    each_edge(lambda i: edge(i).wait_send(), False)

    def receive_edge(i):
        es, et = EDGES[i]
        edge_back(i).wait_recv()
        at = per - 1 if et < 0 else 0
        for c in range(3):
            out_ref[c, at : at + 1, :] += from_edge[i, c : c + 1, :]

    def receive(i):
        back(i).wait_recv()
        out_ref[...] += from_strip[i]

    each_edge(receive_edge, True)
    each_side(receive, True)
    each_edge(lambda i: edge_back(i).wait_send(), False)
    each_side(lambda i: back(i).wait_send(), False)


def on_device(coords, displacement, pairs, intact):
    per, points = coords.shape[0], coords.shape[2]
    pair_count = pairs.shape[0]
    groups = math.gcd(pair_count, 8)
    slots = 3 * per + BLOCK
    half = points // 2
    wholes = -(-per // half)
    f32 = jnp.float32
    hbm = pl.BlockSpec(memory_space=pltpu.HBM)
    total = pl.pallas_call(
        force_kernel,
        in_specs=[hbm] * 4,
        out_specs=pl.BlockSpec(memory_space=pltpu.VMEM),
        out_shape=pltpu.VMEM((3, per, points), f32),
        scratch_shapes=[
            pltpu.VMEM((2 * BLOCK, pair_count), jnp.int32),
            pltpu.SMEM((2 * BLOCK, pair_count), jnp.int32),
            pltpu.VMEM((2, pair_count), jnp.int32),
            pltpu.VMEM((4, BLOCK, points), jnp.int32),
            pltpu.VMEM((BLOCK, slots, points), f32),
            pltpu.VMEM((BLOCK, slots, points), f32),
            pltpu.VMEM((2, BLOCK, points), f32),
            pltpu.VMEM((len(EDGES), BLOCK, points), f32),
            pltpu.VMEM(intact.shape, jnp.int32),
            pltpu.VMEM((pair_count, half, points), f32),
            pltpu.VMEM((per, BLOCK, points), f32),
            pltpu.VMEM((2 * per, BLOCK, points), f32),
            pltpu.VMEM((4 * per, 2 * BLOCK, points), jnp.bfloat16),
            pltpu.VMEM((2 * wholes, BLOCK, half, points), f32),
            pltpu.VMEM((pair_count, 3, half, points), f32),
            pltpu.VMEM((pair_count, 3, half, points), f32),
            pltpu.VMEM((pair_count, BLOCK, points), f32),
            pltpu.VMEM((pair_count, half, points), f32),
            pltpu.VMEM((pair_count, half, points), f32),
            pltpu.VMEM((pair_count, half, points), f32),
            pltpu.VMEM((pair_count, points, points), jnp.bfloat16),
            pltpu.VMEM((3, pair_count, points), f32),
            pltpu.VMEM((2, 3, per, points), f32),
            pltpu.VMEM((len(EDGES), BLOCK, points), f32),
            pltpu.VMEM((2, 3, per, points), f32),
            pltpu.VMEM((len(EDGES), BLOCK, points), f32),
            pltpu.SemaphoreType.DMA((3,)),
            pltpu.SemaphoreType.DMA,
            pltpu.SemaphoreType.DMA((groups,)),
            pltpu.SemaphoreType.DMA((4,)),
            pltpu.SemaphoreType.DMA((4,)),
            pltpu.SemaphoreType.DMA((len(EDGES),)),
            pltpu.SemaphoreType.DMA((len(EDGES),)),
            pltpu.SemaphoreType.DMA((2,)),
            pltpu.SemaphoreType.DMA((2,)),
            pltpu.SemaphoreType.DMA((len(EDGES),)),
            pltpu.SemaphoreType.DMA((len(EDGES),)),
        ],
        compiler_params=pltpu.CompilerParams(
            collective_id=0, has_side_effects=True, vmem_limit_bytes=60 * 1024 * 2**10
        ),
    )(pairs.T, coords.transpose(1, 0, 2), displacement.transpose(1, 0, 2), intact)
    return jnp.transpose(total, (1, 0, 2))


def solution(mesh):
    placed = (
        P(("strip", "tile"), None, None),
        P(("strip", "tile"), None, None),
        P(("strip", "tile"), None),
        P(("strip", "tile"), None, None),
    )
    return jax.shard_map(
        on_device,
        mesh=mesh,
        in_specs=placed,
        out_specs=P(("strip", "tile"), None, None),
        check_vma=False,
    )
```
